8 devices in a mesh: dp: 1 (over z), wg: 8 (over y, x, core).
Axes of the slice: x: 2, y: 2, z: 1, core: 2. Of those that a mesh axis runs over, the one named last changes fastest.
Arguments:
- x: bfloat16 [8, 256, 2560], P(('dp', 'wg'))
- positions: int32 [256], P('dp')
- prompt_len: int32 [8], P(('dp', 'wg'))
- ln_attn: bfloat16 [2, 2, 2560], P(None, None, 'wg')
- ln_mlp: bfloat16 [2, 2, 2560], P(None, None, 'wg')
- w_qkv: bfloat16 [2, 2560, 7680], P(None, None, 'wg')
- w_out: bfloat16 [2, 32, 80, 2560], P(None, None, None, 'wg')
- w_up: bfloat16 [2, 2560, 10240], P(None, None, 'wg')
- w_down: bfloat16 [2, 10240, 2560], P(None, None, 'wg')
Outputs:
- output 1: bfloat16 [8, 256, 2560], P(('dp', 'wg'))
- output 2: bfloat16 [2, 8, 256, 32, 80], P(None, ('dp', 'wg'))
- output 3: bfloat16 [2, 8, 256, 32, 80], P(None, ('dp', 'wg'))
All inputs are finite; a program needn't handle non-finite values.
Results may differ from the reference program's by a relative error of at most 0.0144262.
Values are sent between devices in bfloat16 or wider.
A program may use at most 1 GiB of HBM per device.

```python
import jax
import jax.numpy as jnp
from jax import lax

D = 2560
HEADS = 32
KV_HEADS = 32
HEAD = 80
FF = 10240
LAYERS = 2
BATCH = 8
SEQ = 256

Q_PER = HEADS // KV_HEADS
QKV_COLS = KV_HEADS * (Q_PER + 2) * HEAD
EPSILON = 1e-5
ROPE_BASE = 10000.0


def norm_table(key_gain, key_bias):
    gain_rows = 1.0 + 0.25 * jax.random.normal(key_gain, (LAYERS, D), jnp.float32)
    bias_rows = 0.25 * jax.random.normal(key_bias, (LAYERS, D), jnp.float32)
    return jnp.stack([gain_rows, bias_rows], axis=1).astype(jnp.bfloat16)


def setup_inputs(seed: int = 0, part: int = 0) -> dict:
    root_key = jax.random.key(seed)
    part_key = jax.random.fold_in(root_key, part)
    key_x, key_pos, key_len = jax.random.split(part_key, 3)
    shared = jax.random.split(jax.random.key(seed + 1), 8)
    x = jax.random.normal(key_x, (BATCH, SEQ, D), jnp.float32).astype(jnp.bfloat16)
    pos_start = jax.random.randint(key_pos, (), 0, 2048, dtype=jnp.int32)
    positions = pos_start + jnp.arange(SEQ, dtype=jnp.int32)
    raw_lens = jax.random.randint(key_len, (BATCH,), max(1, SEQ // 4), SEQ + 1, dtype=jnp.int32)
    prompt_len = raw_lens.at[0].set(SEQ)
    col_gain = jnp.concatenate([jnp.full((Q_PER,), 2.0, jnp.float32), jnp.ones((2,), jnp.float32)])
    qkv_base = jax.random.normal(shared[4], (LAYERS, D, KV_HEADS, Q_PER + 2, HEAD), jnp.float32)
    w_qkv = (qkv_base * col_gain[:, None] * D ** -0.5).reshape(LAYERS, D, QKV_COLS).astype(jnp.bfloat16)
    w_out = (jax.random.normal(shared[5], (LAYERS, HEADS, HEAD, D), jnp.float32) * (2.0 * (HEADS * HEAD) ** -0.5)).astype(jnp.bfloat16)
    w_up = (jax.random.normal(shared[6], (LAYERS, D, FF), jnp.float32) * D ** -0.5).astype(jnp.bfloat16)
    w_down = (jax.random.normal(shared[7], (LAYERS, FF, D), jnp.float32) * FF ** -0.5).astype(jnp.bfloat16)
    return {'x': x, 'positions': positions, 'prompt_len': prompt_len, 'ln_attn': norm_table(shared[0], shared[1]), 'ln_mlp': norm_table(shared[2], shared[3]), 'w_qkv': w_qkv, 'w_out': w_out, 'w_up': w_up, 'w_down': w_down}


def layer_norm(tok_rows, norm_params):
    rows_f32 = tok_rows.astype(jnp.float32)
    row_mean = jnp.mean(rows_f32, axis=-1, keepdims=True)
    centered = rows_f32 - row_mean
    row_var = jnp.mean(centered * centered, axis=-1, keepdims=True)
    normed = centered * lax.rsqrt(row_var + EPSILON)
    return (normed * norm_params[0].astype(jnp.float32) + norm_params[1].astype(jnp.float32)).astype(jnp.bfloat16)


def rotary_tables(positions):
    half_dim = HEAD // 2
    inv_freq = ROPE_BASE ** (-jnp.arange(half_dim, dtype=jnp.float32) * 2.0 / HEAD)
    angles = positions.astype(jnp.float32)[:, None] * inv_freq[None, :]
    return jnp.cos(angles), jnp.sin(angles)


def apply_rotary(vec, cos_table, sin_table):
    half_dim = vec.shape[-1] // 2
    vec_f32 = vec.astype(jnp.float32)
    first_half = vec_f32[..., :half_dim]
    second_half = vec_f32[..., half_dim:]
    return jnp.concatenate([first_half * cos_table - second_half * sin_table, second_half * cos_table + first_half * sin_table], axis=-1).astype(jnp.bfloat16)


def prompt_layer(tok_rows, length, cos_table, sin_table, weights):
    ln_a, ln_m, w_qkv, w_out, w_up, w_down = weights
    h_attn = layer_norm(tok_rows, ln_a)
    h_mlp = layer_norm(tok_rows, ln_m)
    qkv_rows = jnp.dot(h_attn, w_qkv, preferred_element_type=jnp.float32).astype(jnp.bfloat16)
    grouped = qkv_rows.reshape(SEQ, KV_HEADS, Q_PER + 2, HEAD)
    query_rot = apply_rotary(grouped[:, :, :Q_PER, :], cos_table[:, None, None, :], sin_table[:, None, None, :])
    key_rot = apply_rotary(grouped[:, :, Q_PER, :], cos_table[:, None, :], sin_table[:, None, :])
    value_rows = grouped[:, :, Q_PER + 1, :]
    scores = jnp.einsum('qgph,kgh->gpqk', query_rot.astype(jnp.float32), key_rot.astype(jnp.float32)) * HEAD ** -0.5
    q_index = jnp.arange(SEQ)[:, None]
    k_index = jnp.arange(SEQ)[None, :]
    allowed = (k_index <= q_index) & (k_index < length)
    scores = jnp.where(allowed, scores, -1e30)
    prob_bf16 = jax.nn.softmax(scores, axis=-1).astype(jnp.bfloat16)
    context = jnp.einsum('gpqk,kgh->qgph', prob_bf16.astype(jnp.float32), value_rows.astype(jnp.float32)).astype(jnp.bfloat16)
    attn_out = jnp.dot(context.reshape(SEQ, HEADS * HEAD), w_out.reshape(HEADS * HEAD, D), preferred_element_type=jnp.float32)
    hidden = jax.nn.gelu(jnp.dot(h_mlp, w_up, preferred_element_type=jnp.float32), approximate=False).astype(jnp.bfloat16)
    mlp_out = jnp.dot(hidden, w_down, preferred_element_type=jnp.float32)
    new_rows = (tok_rows.astype(jnp.float32) + attn_out + mlp_out).astype(jnp.bfloat16)
    return new_rows, key_rot, value_rows


def reference(x, positions, prompt_len, ln_attn, ln_mlp, w_qkv, w_out, w_up, w_down):
    cos_table, sin_table = rotary_tables(positions)
    stacked = (ln_attn, ln_mlp, w_qkv, w_out, w_up, w_down)

    def one_prompt(prompt_item):
        tok_rows, length = prompt_item

        def layer_step(carry_rows, weights):
            new_rows, key_rot, value_rows = prompt_layer(carry_rows, length, cos_table, sin_table, weights)
            return new_rows, (key_rot, value_rows)

        final_rows, (key_layers, value_layers) = lax.scan(layer_step, tok_rows, stacked)
        return final_rows, key_layers, value_layers

    y, key_cache, value_cache = lax.map(one_prompt, (x, prompt_len))
    return y, jnp.swapaxes(key_cache, 0, 1), jnp.swapaxes(value_cache, 0, 1)
```

```python
import jax
import jax.numpy as jnp
from jax import lax
from jax.sharding import PartitionSpec as P

EPSILON = 1e-5
ROPE_BASE = 10000.0
F32 = jnp.float32
BF16 = jnp.bfloat16


def exchange(v, s, n):
    return lax.ppermute(v, 'wg', [(i, i ^ s) for i in range(n)])


def layer_norm_pair(rows, gain_a, bias_a, gain_m, bias_m):
    rows_f32 = rows.astype(F32)
    row_mean = jnp.mean(rows_f32, axis=-1, keepdims=True)
    centered = rows_f32 - row_mean
    row_var = jnp.mean(centered * centered, axis=-1, keepdims=True)
    normed = centered * lax.rsqrt(row_var + EPSILON)
    return (normed * gain_a + bias_a).astype(BF16), (normed * gain_m + bias_m).astype(BF16)


def rotary_tables(pos_rows, head_dim):
    half_dim = head_dim // 2
    inv_freq = ROPE_BASE ** (-jnp.arange(half_dim, dtype=F32) * 2.0 / head_dim)
    angles = pos_rows.astype(F32)[..., None] * inv_freq
    return jnp.cos(angles), jnp.sin(angles)


def apply_rotary(vec, cos_table, sin_table):
    half_dim = vec.shape[-1] // 2
    vec_f32 = vec.astype(F32)
    first_half = vec_f32[..., :half_dim]
    second_half = vec_f32[..., half_dim:]
    return jnp.concatenate([first_half * cos_table - second_half * sin_table, second_half * cos_table + first_half * sin_table], axis=-1).astype(BF16)


def attention(qkv, lens, cos_table, sin_table, heads, head_dim):
    b, s, _ = qkv.shape
    grouped = qkv.reshape(b, s, heads, 3, head_dim)
    ct, st = cos_table[None, :, None, :], sin_table[None, :, None, :]
    q = apply_rotary(grouped[:, :, :, 0], ct, st)
    k = apply_rotary(grouped[:, :, :, 1], ct, st)
    v = grouped[:, :, :, 2]
    scores = jnp.einsum('bqhd,bkhd->bhqk', q, k, preferred_element_type=F32) * head_dim ** -0.5
    q_index = jnp.arange(s)[:, None]
    k_index = jnp.arange(s)[None, :]
    allowed = (k_index <= q_index)[None] & (k_index[None] < lens[:, None, None])
    scores = jnp.where(allowed[:, None], scores, -1e30)
    prob = jax.nn.softmax(scores, axis=-1).astype(BF16)
    ctx = jnp.einsum('bhqk,bkhd->bqhd', prob, v, preferred_element_type=F32).astype(BF16)
    return ctx.reshape(b, s, heads * head_dim), jnp.stack([k.reshape(b, s, -1), v.reshape(b, s, -1)], axis=1)


def solution(mesh):
    n = mesh.shape['wg']
    batch_spec = P(('dp', 'wg'))
    col_spec = P(None, None, 'wg')
    out_spec = P(None, None, None, 'wg')
    cache_spec = P(None, ('dp', 'wg'))

    def local_program(x, positions, prompt_len, ln_attn, ln_mlp, w_qkv, w_out, w_up, w_down):
        layers, d_model, _ = w_qkv.shape
        n_heads, head_dim = w_out.shape[1], w_out.shape[2]
        heads = n_heads // n
        seq = x.shape[1]
        ctx_cols = heads * head_dim
        hid_cols = w_up.shape[2]
        me = lax.axis_index('wg')
        ybit = me // 4
        xbit = (me // 2) % 2
        cbit = me % 2
        qid = me % 4
        upper = ybit == 1
        cos_table, sin_table = rotary_tables(positions, head_dim)
        ln_all = lax.all_gather(jnp.concatenate([ln_attn, ln_mlp], axis=1), 'wg', axis=2, tiled=True).astype(F32)
        len_all = lax.all_gather(prompt_len, 'wg', axis=0, tiled=True)

        def ordered(own, other, axis):
            return jnp.concatenate([jnp.where(upper, other, own), jnp.where(upper, own, other)], axis=axis)

        def second_weights(l):
            wd = w_down[l].reshape(n, hid_cols, -1)
            wo = w_out[l].reshape(n, ctx_cols, -1)
            pieces = []
            for r in range(4):
                near, far = me ^ r, me ^ r ^ 4
                part = jnp.concatenate([
                    lax.dynamic_index_in_dim(wd, near, 0, False), lax.dynamic_index_in_dim(wo, near, 0, False),
                    lax.dynamic_index_in_dim(wd, far, 0, False), lax.dynamic_index_in_dim(wo, far, 0, False)], axis=0)
                pieces.append(exchange(part, r, n) if r else part)
            a = [jnp.where(cbit == 1, pieces[i ^ 1], pieces[i]) for i in range(4)]
            b = [jnp.where(xbit == 1, a[i ^ 2], a[i]) for i in range(4)]
            w = jnp.concatenate(b, axis=1)
            blk = hid_cols + ctx_cols
            return w[:hid_cols], w[hid_cols:blk], w[blk:blk + hid_cols], w[blk + hid_cols:]

        weights2 = [second_weights(l) for l in range(layers)]

        own = x[0]
        from_y = exchange(own, 4, n)
        from_x = exchange(own, 2, n)
        half = seq // 2
        diag_a = exchange(from_y[:half], 2, n)
        diag_b = exchange(from_x[half:], 4, n)
        diag = jnp.concatenate([diag_a, diag_b], axis=0)
        c0 = ordered(own[None], from_y[None], 0)
        c2 = ordered(from_x[None], diag[None], 0)
        chunks = {0: c0, 2: c2, 1: exchange(c0, 1, n), 3: exchange(c2, 1, n)}
        key_list, value_list = [], []
        for l in range(layers):
            gain_a, bias_a, gain_m, bias_m = (ln_all[l, i] for i in range(4))
            wd0, wo0, wd1, wo1 = weights2[l]
            kv, part = {}, {}
            for r in (3, 2, 1, 0):
                h_attn, h_mlp = layer_norm_pair(chunks[r], gain_a, bias_a, gain_m, bias_m)
                hidden = jax.nn.gelu(jnp.einsum('bsd,df->bsf', h_mlp, w_up[l], preferred_element_type=F32), approximate=False).astype(BF16)
                hidden_y = exchange(hidden, 4, n)
                qkv = jnp.einsum('bsd,df->bsf', h_attn, w_qkv[l], preferred_element_type=F32).astype(BF16)
                lens = jnp.stack([len_all[qid ^ r], len_all[(qid ^ r) + 4]])
                ctx, kv[r] = attention(qkv, lens, cos_table, sin_table, heads, head_dim)
                ctx_y = exchange(ctx, 4, n)
                dot = lambda p, w: jnp.einsum('bsf,fd->bsd', p, w, preferred_element_type=F32)
                part[r] = dot(hidden, wd0) + dot(ctx, wo0) + dot(hidden_y, wd1) + dot(ctx_y, wo1)
            far = part[2] + exchange(part[3], 1, n)
            near = part[0] + exchange(part[1], 1, n)
            total = near + exchange(far, 2, n)
            c0 = chunks[0]
            res = jnp.where(upper, c0[..., d_model // 2:], c0[..., :d_model // 2])
            new = (res.astype(F32) + total).astype(BF16)
            if l + 1 < layers:
                from_y = exchange(new, 4, n)
                from_x = exchange(new, 2, n)
                diag = jnp.stack([exchange(from_y[0], 2, n), exchange(from_x[1], 4, n)])
                c0 = ordered(new, from_y, 2)
                c2 = ordered(from_x, diag, 2)
                chunks = {0: c0, 2: c2, 1: exchange(c0, 1, n), 3: exchange(c2, 1, n)}
            else:
                mine = jnp.where(upper, new[1], new[0])
                give = jnp.where(upper, new[0], new[1])
                y = ordered(mine, exchange(give, 4, n), 1)[None]
            buf = jnp.zeros((n, 2, seq, ctx_cols), BF16)
            for s in range(n):
                piece = lax.dynamic_index_in_dim(kv[s % 4], ybit ^ (s // 4), 0, False)
                piece = exchange(piece, s, n) if s else piece
                buf = lax.dynamic_update_index_in_dim(buf, piece, me ^ s, 0)
            cache = buf.reshape(n, 2, seq, heads, head_dim).transpose(1, 2, 0, 3, 4).reshape(2, seq, n_heads, head_dim)
            key_list.append(cache[0])
            value_list.append(cache[1])
        return y, jnp.stack(key_list)[:, None], jnp.stack(value_list)[:, None]

    return jax.shard_map(local_program, mesh=mesh, in_specs=(batch_spec, P('dp'), batch_spec, col_spec, col_spec, col_spec, out_spec, col_spec, col_spec), out_specs=(batch_spec, cache_spec, cache_spec), check_vma=False)
```

```python
import jax
import jax.numpy as jnp
from jax import lax
from jax.experimental import pallas as pl
from jax.experimental.pallas import tpu as pltpu
from jax.sharding import PartitionSpec as P

EPSILON = 1e-5
ROPE_BASE = 10000.0
F32 = jnp.float32
BF16 = jnp.bfloat16
MESH = pl.DeviceIdType.MESH
NT = (((1,), (1,)), ((), ()))
TN = (((0,), (0,)), ((), ()))
TT = (((0,), (1,)), ((), ()))


def flip(v, s):
    if s & 1:
        v = v + 1 - 2 * (v % 2)
    if s & 2:
        v = v + 2 - 4 * ((v // 2) % 2)
    if s & 4:
        v = v + 4 - 8 * ((v // 4) % 2)
    return v


def make_kernel(cfg):
    n, layers, seq, d, heads, hd, hid = (cfg[k] for k in ('n', 'layers', 'seq', 'd', 'heads', 'hd', 'hid'))
    two = 2 * seq
    cc = heads * hd
    half_d = d // 2
    hs = seq // 2
    slot = 3 * hd
    half_hd = hd // 2
    tile = 256
    hid_tiles, out_tiles = hid // tile, half_d // tile
    ncols = d // n
    win = ncols + 64

    def kernel(x_ref, wq_ref, wu_ref, wd_ref, wo_ref, ln_ref, cos_ref, sin_ref,
               y_ref, kv_ref, xg_ref, w2_ref, hrec_ref, crec_ref,
               wq, wu, w2v, xbuf, abuf, mbuf, hbuf, hr, kvb, cbuf, p2, p31, p0, pd3, pd1, px, nbuf, lnrec, lnf,
               ssem, rsem, lsem):
        me = lax.axis_index('wg')
        yb = me // 4
        q = me % 4
        row = pl.multiple_of(seq * yb, seq)
        orow = pl.multiple_of(seq * (1 - yb), seq)
        ycol = pl.multiple_of(half_d * yb, half_d)
        ocol = pl.multiple_of(half_d * (1 - yb), half_d)
        counter = [0, 0]

        def take(k=1):
            counter[0] += k
            return counter[0] - k

        def rc(src, dst, s, idx=None):
            i = take() if idx is None else idx
            return pltpu.make_async_remote_copy(src_ref=src, dst_ref=dst, send_sem=ssem.at[i], recv_sem=rsem.at[i],
                                                device_id={'wg': flip(me, s)}, device_id_type=MESH)

        def lc(src, dst):
            counter[1] += 1
            return pltpu.make_async_copy(src, dst, lsem.at[counter[1] - 1])

        def start(*cs):
            for c in cs:
                c.start()
            return cs

        def waits(cs):
            for c in cs:
                c.wait_send()

        def recvs(cs):
            for c in cs:
                c.wait_recv()

        def waitl(cs):
            for c in cs:
                c.wait()

        barrier = pltpu.get_barrier_semaphore()
        for s in range(1, n):
            pl.semaphore_signal(barrier, inc=1, device_id={'wg': flip(me, s)}, device_id_type=MESH)
        pl.semaphore_wait(barrier, n - 1)

        sent = []
        lnc = [rc(ln_ref, lnrec.at[me], s) for s in range(1, n)]
        start(*lnc)
        lnl = start(lc(ln_ref, lnrec.at[me]))

        def load_first(l):
            return start(lc(wq_ref.at[l], wq), lc(wu_ref.at[l], wu))

        def gather0():
            xt, g = x_ref, xg_ref.at[0]
            y1 = rc(xt.at[pl.ds(0, hs)], g.at[0, pl.ds(row, hs)], 4)
            y2 = rc(xt.at[pl.ds(hs, hs)], g.at[0, pl.ds(row + hs, hs)], 4)
            x1 = rc(xt.at[pl.ds(hs, hs)], g.at[2, pl.ds(row + hs, hs)], 2)
            x2 = rc(xt.at[pl.ds(0, hs)], g.at[2, pl.ds(row, hs)], 2)
            c0 = rc(xt, g.at[1, pl.ds(row, seq)], 1)
            start(y1, x1, y2, x2, c0)
            y1.wait_recv()
            rx = rc(g.at[0, pl.ds(orow, hs)], g.at[2, pl.ds(orow, hs)], 2)
            rx.start()
            x1.wait_recv()
            ry = rc(g.at[2, pl.ds(row + hs, hs)], g.at[2, pl.ds(row + hs, hs)], 4)
            ry.start()
            y2.wait_recv()
            c1 = rc(g.at[0, pl.ds(orow, seq)], g.at[1, pl.ds(orow, seq)], 1)
            c1.start()
            sent.extend([y1, y2, x1, x2, c0, rx, ry, c1])

            def rest():
                x2.wait_recv()
                c2 = rc(g.at[2, pl.ds(row, seq)], g.at[3, pl.ds(row, seq)], 1)
                c2.start()
                recvs([rx, ry])
                c3 = rc(g.at[2, pl.ds(orow, seq)], g.at[3, pl.ds(orow, seq)], 1)
                c3.start()
                sent.extend([c2, c3])
                return [c2, c3]
            return rest, [c0, c1]

        def gather1(l):
            g = xg_ref.at[l]
            lo, hi = pl.ds(0, seq), pl.ds(seq, seq)
            yc, oc = pl.ds(ycol, half_d), pl.ds(ocol, half_d)
            y1 = rc(nbuf.at[lo], g.at[0, lo, yc], 4)
            y2 = rc(nbuf.at[hi], g.at[0, hi, yc], 4)
            x1 = rc(nbuf.at[hi], g.at[2, hi, yc], 2)
            x2 = rc(nbuf.at[lo], g.at[2, lo, yc], 2)
            start(y1, x1, y2, x2)
            own = start(lc(nbuf, g.at[0, :, yc]))
            y1.wait_recv()
            rx = rc(g.at[0, lo, oc], g.at[2, lo, oc], 2)
            rx.start()
            x1.wait_recv()
            ry = rc(g.at[2, hi, yc], g.at[2, hi, yc], 4)
            ry.start()
            y2.wait_recv()
            waitl(own)
            c1 = rc(g.at[0], g.at[1], 1)
            c1.start()
            sent.extend([y1, y2, x1, x2, rx, ry, c1])

            def rest():
                recvs([x2, rx, ry])
                c3 = rc(g.at[2], g.at[3], 1)
                c3.start()
                sent.append(c3)
                return [c3]
            return rest, [c1]

        def send_weights(l):
            rows = pl.ds(pl.multiple_of(cc * q, 64), cc)
            out = []
            for r in (2, 3, 1):
                t = flip(me, r)
                ty = flip(t, 4)
                out.append(rc(wd_ref.at[l, :, pl.ds(pl.multiple_of(hid * t, 128), hid)], w2_ref.at[l, rows, pl.ds(0, hid)], r))
                out.append(rc(wd_ref.at[l, :, pl.ds(pl.multiple_of(hid * ty, 128), hid)], w2_ref.at[l, rows, pl.ds(hid, hid)], r))
                out.append(rc(wo_ref.at[l, t % 4], w2_ref.at[l, rows, pl.ds(2 * hid, 2 * cc)], r))
            start(*out)
            sent.extend(out)
            return out

        def own_weights(l):
            rows = pl.ds(pl.multiple_of(cc * q, 64), cc)
            return start(
                lc(wd_ref.at[l, :, pl.ds(pl.multiple_of(hid * me, 128), hid)], w2v.at[rows, pl.ds(0, hid)]),
                lc(wd_ref.at[l, :, pl.ds(pl.multiple_of(hid * flip(me, 4), 128), hid)], w2v.at[rows, pl.ds(hid, hid)]),
                lc(wo_ref.at[l, q], w2v.at[rows, pl.ds(2 * hid, 2 * cc)]))

        def other_weights(l, inbound):
            recvs(inbound)
            cs = []
            for r in (1, 2, 3):
                rows = pl.ds(pl.multiple_of(cc * flip(q, r), 64), cc)
                cs.append(lc(w2_ref.at[l, rows], w2v.at[rows]))
            return start(*cs)

        def load_x(l, r):
            if l == 0 and r == 0:
                return start(lc(x_ref, xbuf.at[pl.ds(row, seq)]), lc(xg_ref.at[0, 0, pl.ds(orow, seq)], xbuf.at[pl.ds(orow, seq)]))
            return start(lc(xg_ref.at[l, r], xbuf))

        def norm(l):
            @pl.loop(0, two // 16)
            def _(i):
                rs = pl.ds(pl.multiple_of(i * 16, 16), 16)
                v = xbuf[rs, :].astype(F32)
                cen = v - jnp.mean(v, axis=-1, keepdims=True)
                var = jnp.mean(cen * cen, axis=-1, keepdims=True)
                nrm = cen * lax.rsqrt(var + EPSILON)
                k = 4 * l
                abuf[rs, :] = (nrm * lnf[k:k + 1, :] + lnf[k + 1:k + 2, :]).astype(BF16)
                mbuf[rs, :] = (nrm * lnf[k + 2:k + 3, :] + lnf[k + 3:k + 4, :]).astype(BF16)

        def h_copy(l, r, t, base):
            cs = pl.ds(pl.multiple_of(t * tile, tile), tile)
            return rc(hbuf.at[r, :, cs], hrec_ref.at[l, r, :, cs], 4, base + t)

        def up(l, r, base):
            @pl.loop(0, hid_tiles)
            def _(t):
                cs = pl.ds(pl.multiple_of(t * tile, tile), tile)
                u = jnp.dot(mbuf[...], wu[:, cs], preferred_element_type=F32)
                hbuf[r, :, cs] = (0.5 * u * (1.0 + lax.erf(u * (0.5 ** 0.5)))).astype(BF16)
                h_copy(l, r, t, base).start()

        def attend(l, r):
            kidx = lax.broadcasted_iota(jnp.int32, (seq, seq), 0)
            qidx = lax.broadcasted_iota(jnp.int32, (seq, seq), 1)
            causal = kidx <= qidx
            kf = kidx.astype(F32)

            @pl.loop(0, heads)
            def _(h):
                t = lax.dot_general(wq[pl.ds(pl.multiple_of(h * slot, 16), slot), :], abuf[...], NT, preferred_element_type=F32)
                t = t.astype(BF16).astype(F32)
                cs, sn = cos_ref[...], sin_ref[...]

                def turn(v):
                    a, b = v[:half_hd], v[half_hd:]
                    return jnp.concatenate([a * cs - b * sn, b * cs + a * sn], axis=0).astype(BF16)
                qr, kr, vr = turn(t[:hd]), turn(t[hd:2 * hd]), t[2 * hd:].astype(BF16)
                hrow = pl.ds(pl.multiple_of(h * hd, 16), hd)
                kvb[r, 0, hrow, :] = kr
                kvb[r, 1, hrow, :] = vr
                crow = pl.ds(pl.multiple_of(cc * yb + h * hd, 16), hd)
                for j in range(2):
                    ps = slice(j * seq, (j + 1) * seq)
                    s = lax.dot_general(kr[:, ps], qr[:, ps], TN, preferred_element_type=F32) * hd ** -0.5
                    plen = lnrec[flip(q, r) + 4 * j, 8:9, 0:seq].astype(F32)
                    s = jnp.where(causal & (kf < plen), s, -1e30)
                    e = jnp.exp(s - jnp.max(s, axis=0, keepdims=True))
                    p = (e / jnp.sum(e, axis=0, keepdims=True)).astype(BF16)
                    cbuf[r, crow, ps] = jnp.dot(vr[:, ps], p, preferred_element_type=F32).astype(BF16)

        def first(l, r, prev):
            xs = load_x(l, r)
            if prev:
                waits(prev)
            waitl(xs)
            norm(l)
            base = take(hid_tiles)
            up(l, r, base)
            attend(l, r)
            crows = pl.ds(pl.multiple_of(cc * yb, 64), cc)
            c = rc(cbuf.at[r, crows], crec_ref.at[l, r], 4)
            c.start()
            hcs = [h_copy(l, r, t, base) for t in range(hid_tiles)]
            return hcs, c

        def kv_send(l, r, ys):
            j = yb if ys == 0 else 1 - yb
            src = kvb.at[r, :, :, pl.ds(pl.multiple_of(seq * j, seq), seq)]
            dst = kv_ref.at[l, :, pl.ds(pl.multiple_of(cc * me, 64), cc), :]
            s = 4 * ys + r
            c = lc(src, dst) if s == 0 else rc(src, dst, s)
            c.start()
            return c

        def second(l, r, hcs, c, dst, send_to, wait_before):
            recvs(hcs)
            c.wait_recv()
            orows = pl.ds(pl.multiple_of(cc * (1 - yb), 64), cc)
            cs = start(lc(hrec_ref.at[l, r], hr), lc(crec_ref.at[l, r], cbuf.at[r, orows]))
            waitl(cs)
            if wait_before:
                waits(wait_before)
            base = take(out_tiles) if send_to is not None else None

            def p_copy(t):
                ts = pl.ds(pl.multiple_of(t * tile, tile), tile)
                return rc(dst.at[:, ts], send_to.at[:, ts], 1, base + t)

            @pl.loop(0, out_tiles)
            def _(t):
                ts = pl.ds(pl.multiple_of(t * tile, tile), tile)
                acc = lax.dot_general(hbuf[r], w2v[ts, 0:hid], NT, preferred_element_type=F32)
                acc = acc + lax.dot_general(hr[...], w2v[ts, hid:2 * hid], NT, preferred_element_type=F32)
                acc = acc + lax.dot_general(cbuf[r], w2v[ts, 2 * hid:], TT, preferred_element_type=F32)
                dst[:, ts] = acc
                if send_to is not None:
                    p_copy(t).start()
            return [p_copy(t) for t in range(out_tiles)] if send_to is not None else []

        rest, near = gather0()
        lw = load_first(0)
        res0 = start(lc(x_ref.at[:, pl.ds(ycol, half_d)], nbuf.at[pl.ds(row, seq)]),
                     lc(xg_ref.at[0, 0, pl.ds(orow, seq), pl.ds(ycol, half_d)], nbuf.at[pl.ds(orow, seq)]))
        recvs(lnc)
        waitl(lnl)
        lnf[...] = jnp.zeros_like(lnf)
        for e in range(n):
            lo = ncols * e - 64 * (e % 2)
            lnf[:, lo:lo + win] += lnrec[e].astype(F32)
        wait_prev = {r: [] for r in range(4)}
        p_prev = {'p2': [], 'p31': []}
        kv_local = []
        for l in range(layers):
            inbound = send_weights(l)
            w_own = own_weights(l)
            waitl(lw)
            hc, xc = {}, {}
            hc[0], xc[0] = first(l, 0, wait_prev[0])
            far = rest()
            hc[2], xc[2] = first(l, 2, wait_prev[2])
            recvs(far)
            hc[3], xc[3] = first(l, 3, wait_prev[3])
            recvs(near)
            hc[1], xc[1] = first(l, 1, wait_prev[1])
            kvs = {r: [] for r in range(4)}
            for r in range(4):
                kvs[r].append(kv_send(l, r, 1))
            kvs[1].append(kv_send(l, 1, 0))
            if l + 1 < layers:
                lw = load_first(l + 1)
            w_in = other_weights(l, inbound)
            waitl(w_own)
            waitl(w_in)
            second(l, 2, hc[2], xc[2], p2, None, p_prev['p2'])
            c3 = second(l, 3, hc[3], xc[3], p31, pd3, p_prev['p31'])
            xbase = take(out_tiles)

            def x_copy(t):
                ts = pl.ds(t * tile, tile)
                return rc(p2.at[:, ts], px.at[:, ts], 2, xbase + t)
            for t in range(out_tiles):
                ts = slice(t * tile, (t + 1) * tile)
                c3[t].wait_recv()
                p2[:, ts] += pd3[:, ts]
                x_copy(t).start()
            xcs = [x_copy(t) for t in range(out_tiles)]
            kvs[2].append(kv_send(l, 2, 0))
            kvs[3].append(kv_send(l, 3, 0))
            loc = kv_send(l, 0, 0)
            c1 = second(l, 1, hc[1], xc[1], p31, pd1, c3)
            second(l, 0, hc[0], xc[0], p0, None, [])
            if l == 0:
                waitl(res0)
            else:
                waits(sent)
                sent.clear()
            for t in range(out_tiles):
                ts = slice(t * tile, (t + 1) * tile)
                c1[t].wait_recv()
                xcs[t].wait_recv()
                total = p0[:, ts] + pd1[:, ts] + px[:, ts]
                nbuf[:, ts] = (nbuf[:, ts].astype(F32) + total).astype(BF16)
            loc.wait()
            if l + 1 < layers:
                waits(sent)
                sent.clear()
                rest, near = gather1(l + 1)
                wait_prev = {r: hc[r] + [xc[r]] + kvs[r] for r in range(4)}
                p_prev = {'p2': xcs, 'p31': c1}
                recvs([c for r in range(4) for c in kvs[r]])
            else:
                fin = rc(nbuf.at[pl.ds(orow, seq)], y_ref.at[:, pl.ds(ycol, half_d)], 4)
                fin.start()
                loc = start(lc(nbuf.at[pl.ds(row, seq)], y_ref.at[:, pl.ds(ycol, half_d)]))
                waits(xcs + c1 + [c for r in range(4) for c in hc[r] + [xc[r]] + kvs[r]])
                recvs([c for r in range(4) for c in kvs[r]])
                fin.wait()
                waitl(loc)
        waits(lnc)
        assert counter[0] <= cfg['n_remote'] and counter[1] <= cfg['n_local'], counter
    return kernel


def solution(mesh):
    n = mesh.shape['wg']
    batch_spec = P(('dp', 'wg'))
    col_spec = P(None, None, 'wg')
    out_spec = P(None, None, None, 'wg')
    cache_spec = P(None, ('dp', 'wg'))

    def local_program(x, positions, prompt_len, ln_attn, ln_mlp, w_qkv, w_out, w_up, w_down):
        layers, d, _ = w_qkv.shape
        n_heads, hd = w_out.shape[1], w_out.shape[2]
        heads = n_heads // n
        seq, hid, cc = x.shape[1], w_up.shape[2], heads * hd
        two, half_d = 2 * seq, d // 2
        me = lax.axis_index('wg')
        cfg = dict(n=n, layers=layers, seq=seq, d=d, heads=heads, hd=hd, hid=hid, n_remote=192, n_local=96)
        half_hd = hd // 2
        inv_freq = ROPE_BASE ** (-jnp.arange(half_hd, dtype=F32) * 2.0 / hd)
        angles = positions.astype(F32)[None, :] * inv_freq[:, None]
        cos_t, sin_t = (jnp.tile(f(angles), (1, 2)) for f in (jnp.cos, jnp.sin))
        ln = jnp.concatenate([ln_attn, ln_mlp], axis=1).reshape(4 * layers, -1)
        wide = jnp.where(me % 2 == 1, jnp.pad(ln, ((0, 0), (64, 0))), jnp.pad(ln, ((0, 0), (0, 64))))
        win = wide.shape[1]
        lens = jnp.broadcast_to(prompt_len.astype(BF16)[:, None], (1, win))
        ln_piece = jnp.concatenate([wide, lens, jnp.zeros((16 - 4 * layers - 1, win), BF16)], axis=0)
        wq_t = w_qkv.transpose(0, 2, 1)
        wd_t = w_down.transpose(0, 2, 1)
        wo_t = w_out.reshape(layers, 2, 4, cc, cc).transpose(0, 2, 4, 1, 3).reshape(layers, 4, cc, 2 * cc)

        hbm = pl.BlockSpec(memory_space=pltpu.MemorySpace.HBM)
        vmem = pl.BlockSpec(memory_space=pltpu.MemorySpace.VMEM)
        sds = jax.ShapeDtypeStruct
        outs = pl.pallas_call(
            make_kernel(cfg),
            out_shape=[
                sds((seq, d), BF16), sds((layers, 2, d, seq), BF16), sds((layers, 4, two, d), BF16),
                sds((layers, half_d, 2 * hid + 2 * cc), BF16), sds((layers, 4, two, hid), BF16), sds((layers, 4, cc, two), BF16)],
            in_specs=[hbm] * 5 + [hbm, vmem, vmem],
            out_specs=[hbm] * 6,
            scratch_shapes=[
                pltpu.VMEM((3 * cc, d), BF16), pltpu.VMEM((d, hid), BF16), pltpu.VMEM((half_d, 2 * hid + 2 * cc), BF16),
                pltpu.VMEM((two, d), BF16), pltpu.VMEM((two, d), BF16), pltpu.VMEM((two, d), BF16),
                pltpu.VMEM((4, two, hid), BF16), pltpu.VMEM((two, hid), BF16),
                pltpu.VMEM((4, 2, cc, two), BF16), pltpu.VMEM((4, 2 * cc, two), BF16),
                pltpu.VMEM((two, half_d), F32), pltpu.VMEM((two, half_d), F32), pltpu.VMEM((two, half_d), F32),
                pltpu.VMEM((two, half_d), F32), pltpu.VMEM((two, half_d), F32), pltpu.VMEM((two, half_d), F32),
                pltpu.VMEM((two, half_d), BF16), pltpu.VMEM((n, 16, win), BF16), pltpu.VMEM((16, d), F32),
                pltpu.SemaphoreType.DMA((cfg['n_remote'],)), pltpu.SemaphoreType.DMA((cfg['n_remote'],)),
                pltpu.SemaphoreType.DMA((cfg['n_local'],))],
            compiler_params=pltpu.CompilerParams(collective_id=0, has_side_effects=True, vmem_limit_bytes=67043328),
        )(x[0], wq_t, w_up, wd_t, wo_t, ln_piece, cos_t, sin_t)
        y, kv = outs[0], outs[1]
        caches = [kv[:, i].reshape(layers, 1, n_heads, hd, seq).transpose(0, 1, 4, 2, 3) for i in range(2)]
        return y[None], caches[0], caches[1]

    return jax.shard_map(local_program, mesh=mesh, in_specs=(batch_spec, P('dp'), batch_spec, col_spec, col_spec, col_spec, out_spec, col_spec, col_spec), out_specs=(batch_spec, cache_spec, cache_spec), check_vma=False)
```

```python
import jax
import jax.numpy as jnp
from jax import lax
from jax.experimental import pallas as pl
from jax.experimental.pallas import tpu as pltpu
from jax.sharding import PartitionSpec as P

EPSILON = 1e-5
ROPE_BASE = 10000.0
F32 = jnp.float32
BF16 = jnp.bfloat16
MESH = pl.DeviceIdType.MESH
NT = (((1,), (1,)), ((), ()))
TN = (((0,), (0,)), ((), ()))
TT = (((0,), (1,)), ((), ()))
HELD = 2


def flip(v, s):
    if s & 1:
        v = v + 1 - 2 * (v % 2)
    if s & 2:
        v = v + 2 - 4 * ((v // 2) % 2)
    if s & 4:
        v = v + 4 - 8 * ((v // 4) % 2)
    return v


def make_kernel(cfg):
    n, layers, seq, d, heads, hd, hid = (cfg[k] for k in ('n', 'layers', 'seq', 'd', 'heads', 'hd', 'hid'))
    two = 2 * seq
    cc = heads * hd
    half_d = d // 2
    hs = seq // 2
    slot = 3 * hd
    half_hd = hd // 2
    tile = 256
    hid_tiles, out_tiles = hid // tile, half_d // tile
    ncols = d // n
    win = ncols + 64

    def kernel(x_ref, wq_ref, wu_ref, wd_ref, wo_ref, ln_ref, cos_ref, sin_ref,
               y_ref, kv_ref, xg_ref, w2_ref, hrec_ref, crec_ref,
               wq, wu, w2v, wob, wot, xbuf, abuf, mbuf, hbuf, hr, kvb, cbuf, p2, p31, p0, pd3, pd1, px, nbuf, lnrec, lnf,
               ssem, rsem, lsem):
        me = lax.axis_index('wg')
        yb = me // 4
        q = me % 4
        row = pl.multiple_of(seq * yb, seq)
        orow = pl.multiple_of(seq * (1 - yb), seq)
        ycol = pl.multiple_of(half_d * yb, half_d)
        ocol = pl.multiple_of(half_d * (1 - yb), half_d)
        counter = [0, 0]

        def take(k=1):
            counter[0] += k
            return counter[0] - k

        def rc(src, dst, s, idx=None):
            i = take() if idx is None else idx
            return pltpu.make_async_remote_copy(src_ref=src, dst_ref=dst, send_sem=ssem.at[i], recv_sem=rsem.at[i],
                                                device_id={'wg': flip(me, s)}, device_id_type=MESH)

        def lc(src, dst):
            counter[1] += 1
            return pltpu.make_async_copy(src, dst, lsem.at[counter[1] - 1])

        def start(*cs):
            for c in cs:
                c.start()
            return cs

        def waits(cs):
            for c in cs:
                c.wait_send()

        def recvs(cs):
            for c in cs:
                c.wait_recv()

        def waitl(cs):
            for c in cs:
                c.wait()

        barrier = pltpu.get_barrier_semaphore()
        for s in range(1, n):
            pl.semaphore_signal(barrier, inc=1, device_id={'wg': flip(me, s)}, device_id_type=MESH)
        pl.semaphore_wait(barrier, n - 1)

        sent = []
        lnc = [rc(ln_ref, lnrec.at[me], s) for s in range(1, n)]
        start(*lnc)
        lnl = start(lc(ln_ref, lnrec.at[me]))

        def load_out(l):
            return start(lc(wo_ref.at[l], wob))

        def turn_out():
            eye = (lax.broadcasted_iota(jnp.int32, (cc, cc), 0) == lax.broadcasted_iota(jnp.int32, (cc, cc), 1)).astype(F32).astype(BF16)
            for i in range(4):
                pair = jnp.concatenate([wob[cc * i:cc * (i + 1), :], wob[cc * (i + 4):cc * (i + 5), :]], axis=0)
                wot[i] = lax.dot_general(eye, pair, NT, preferred_element_type=F32).astype(BF16)

        def load_first(l):
            return start(lc(wq_ref.at[l], wq), lc(wu_ref.at[l], wu))

        def gather0():
            xt, g = x_ref, xg_ref.at[0]
            y1 = rc(xt.at[pl.ds(0, hs)], g.at[0, pl.ds(row, hs)], 4)
            y2 = rc(xt.at[pl.ds(hs, hs)], g.at[0, pl.ds(row + hs, hs)], 4)
            x1 = rc(xt.at[pl.ds(hs, hs)], g.at[2, pl.ds(row + hs, hs)], 2)
            x2 = rc(xt.at[pl.ds(0, hs)], g.at[2, pl.ds(row, hs)], 2)
            c0 = rc(xt, g.at[1, pl.ds(row, seq)], 1)
            start(y1, x1, y2, x2, c0)
            wl = load_out(0)
            waitl(wl)
            turn_out()
            y1.wait_recv()
            rx = rc(g.at[0, pl.ds(orow, hs)], g.at[2, pl.ds(orow, hs)], 2)
            rx.start()
            x1.wait_recv()
            ry = rc(g.at[2, pl.ds(row + hs, hs)], g.at[2, pl.ds(row + hs, hs)], 4)
            ry.start()
            y2.wait_recv()
            c1 = rc(g.at[0, pl.ds(orow, seq)], g.at[1, pl.ds(orow, seq)], 1)
            c1.start()
            sent.extend([y1, y2, x1, x2, c0, rx, ry, c1])

            def rest():
                x2.wait_recv()
                c2 = rc(g.at[2, pl.ds(row, seq)], g.at[3, pl.ds(row, seq)], 1)
                c2.start()
                recvs([rx, ry])
                c3 = rc(g.at[2, pl.ds(orow, seq)], g.at[3, pl.ds(orow, seq)], 1)
                c3.start()
                sent.extend([c2, c3])
                return [c2, c3]
            return rest, [c0, c1]

        def tile_cols(t, base=0):
            off = base + t * tile
            return pl.ds(off if isinstance(off, int) else pl.multiple_of(off, tile), tile)

        def gather1(l, finish):
            g = xg_ref.at[l]
            lo, hi = pl.ds(0, seq), pl.ds(seq, seq)
            ys, xs, own = [], [], []

            def send(t):
                src, dc = nbuf.at[:, tile_cols(t)], tile_cols(t, ycol)
                ys.append(rc(src, g.at[0, :, dc], 4))
                xs.append(rc(src, g.at[2, :, dc], 2))
                own.append(lc(src, g.at[0, :, dc]))
                start(ys[t], xs[t], own[t])
            for t in range(out_tiles):
                finish(t)
                if t:
                    send(t - 1)
            send(out_tiles - 1)
            rx, ry = [], []
            for t in range(out_tiles):
                ys[t].wait_recv()
                oc = tile_cols(t, ocol)
                rx.append(rc(g.at[0, lo, oc], g.at[2, lo, oc], 2))
                rx[t].start()
            waitl(own)
            c1 = rc(g.at[0], g.at[1], 1)
            c1.start()
            sent.extend(ys + xs + rx + [c1])

            def rest():
                for t in range(out_tiles):
                    xs[t].wait_recv()
                    yc = tile_cols(t, ycol)
                    ry.append(rc(g.at[2, hi, yc], g.at[2, hi, yc], 4))
                    ry[t].start()
                recvs(rx + ry)
                c3 = rc(g.at[2], g.at[3], 1)
                c3.start()
                sent.extend(ry + [c3])
                return [c3]
            return rest, [c1]

        def send_weights(l):
            rows = pl.ds(pl.multiple_of(cc * q, 64), cc)
            out = []
            for r in (2, 3, 1):
                t = flip(me, r)
                ty = flip(t, 4)
                out.append(rc(wd_ref.at[l, :, pl.ds(pl.multiple_of(hid * t, 128), hid)], w2_ref.at[l, rows, pl.ds(0, hid)], r))
                out.append(rc(wd_ref.at[l, :, pl.ds(pl.multiple_of(hid * ty, 128), hid)], w2_ref.at[l, rows, pl.ds(hid, hid)], r))
                out.append(rc(wot.at[t % 4], w2_ref.at[l, rows, pl.ds(2 * hid, 2 * cc)], r))
            start(*out)
            sent.extend(out)
            return out

        def own_weights(l):
            rows = pl.ds(pl.multiple_of(cc * q, 64), cc)
            return start(
                lc(wd_ref.at[l, :, pl.ds(pl.multiple_of(hid * me, 128), hid)], w2v.at[rows, pl.ds(0, hid)]),
                lc(wd_ref.at[l, :, pl.ds(pl.multiple_of(hid * flip(me, 4), 128), hid)], w2v.at[rows, pl.ds(hid, hid)]))

        def other_weights(l, inbound):
            recvs(inbound)
            cs = []
            for r in (1, 2, 3):
                rows = pl.ds(pl.multiple_of(cc * flip(q, r), 64), cc)
                cs.append(lc(w2_ref.at[l, rows], w2v.at[rows]))
            return start(*cs)

        def load_x(l, r):
            if l == 0 and r == 0:
                return start(lc(x_ref, xbuf.at[pl.ds(row, seq)]), lc(xg_ref.at[0, 0, pl.ds(orow, seq)], xbuf.at[pl.ds(orow, seq)]))
            return start(lc(xg_ref.at[l, r], xbuf))

        def norm(l):
            @pl.loop(0, two // 16, unroll=4)
            def _(i):
                rs = pl.ds(pl.multiple_of(i * 16, 16), 16)
                v = xbuf[rs, :].astype(F32)
                cen = v - jnp.mean(v, axis=-1, keepdims=True)
                var = jnp.mean(cen * cen, axis=-1, keepdims=True)
                nrm = cen * lax.rsqrt(var + EPSILON)
                k = 4 * l
                abuf[rs, :] = (nrm * lnf[k:k + 1, :] + lnf[k + 1:k + 2, :]).astype(BF16)
                mbuf[rs, :] = (nrm * lnf[k + 2:k + 3, :] + lnf[k + 3:k + 4, :]).astype(BF16)

        def h_copy(l, r, t, base):
            cs = pl.ds(pl.multiple_of(t * tile, tile), tile)
            return rc(hbuf.at[r, :, cs], hrec_ref.at[l, r, :, cs], 4, base + t)

        def up(l, r, base, now):
            @pl.loop(0, hid_tiles)
            def _(t):
                cs = pl.ds(pl.multiple_of(t * tile, tile), tile)
                u = jnp.dot(mbuf[...], wu[:, cs], preferred_element_type=F32)
                hbuf[r, :, cs] = (0.5 * u * (1.0 + lax.erf(u * (0.5 ** 0.5)))).astype(BF16)

                @pl.when((t > 0) & (t <= now))
                def _():
                    h_copy(l, r, t - 1, base).start()
            if now == hid_tiles:
                h_copy(l, r, hid_tiles - 1, base).start()

        def attend(l, r):
            kidx = lax.broadcasted_iota(jnp.int32, (seq, seq), 0)
            qidx = lax.broadcasted_iota(jnp.int32, (seq, seq), 1)
            causal = kidx <= qidx
            kf = kidx.astype(F32)

            @pl.loop(0, heads)
            def _(h):
                t = lax.dot_general(wq[pl.ds(pl.multiple_of(h * slot, 16), slot), :], abuf[...], NT, preferred_element_type=F32)
                t = t.astype(BF16).astype(F32)
                cs, sn = cos_ref[...], sin_ref[...]

                def turn(v):
                    a, b = v[:half_hd], v[half_hd:]
                    return jnp.concatenate([a * cs - b * sn, b * cs + a * sn], axis=0).astype(BF16)
                qr, kr, vr = turn(t[:hd]), turn(t[hd:2 * hd]), t[2 * hd:].astype(BF16)
                hrow = pl.ds(pl.multiple_of(h * hd, 16), hd)
                kvb[r, 0, hrow, :] = kr
                kvb[r, 1, hrow, :] = vr
                crow = pl.ds(pl.multiple_of(cc * yb + h * hd, 16), hd)
                for j in range(2):
                    ps = slice(j * seq, (j + 1) * seq)
                    s = lax.dot_general(kr[:, ps], qr[:, ps], TN, preferred_element_type=F32) * hd ** -0.5
                    plen = lnrec[flip(q, r) + 4 * j, 8:9, 0:seq].astype(F32)
                    s = jnp.where(causal & (kf < plen), s, -1e30)
                    e = jnp.exp(s - jnp.max(s, axis=0, keepdims=True))
                    p = (e / jnp.sum(e, axis=0, keepdims=True)).astype(BF16)
                    cbuf[r, crow, ps] = jnp.dot(vr[:, ps], p, preferred_element_type=F32).astype(BF16)

        def first(l, r, prev, now):
            xs = load_x(l, r)
            if prev:
                waits(prev)
            waitl(xs)
            norm(l)
            base = take(hid_tiles)
            up(l, r, base, now)
            attend(l, r)
            crows = pl.ds(pl.multiple_of(cc * yb, 64), cc)
            c = rc(cbuf.at[r, crows], crec_ref.at[l, r], 4)
            hcs = [h_copy(l, r, t, base) for t in range(hid_tiles)]
            if now == hid_tiles:
                c.start()
            return hcs, c

        def kv_send(l, r, ys):
            j = yb if ys == 0 else 1 - yb
            src = kvb.at[r, :, :, pl.ds(pl.multiple_of(seq * j, seq), seq)]
            dst = kv_ref.at[l, :, pl.ds(pl.multiple_of(cc * me, 64), cc), :]
            s = 4 * ys + r
            c = lc(src, dst) if s == 0 else rc(src, dst, s)
            c.start()
            return c

        def second(l, r, hcs, c, dst, send_to, wait_before):
            recvs(hcs)
            c.wait_recv()
            orows = pl.ds(pl.multiple_of(cc * (1 - yb), 64), cc)
            cs = start(lc(hrec_ref.at[l, r], hr), lc(crec_ref.at[l, r], cbuf.at[r, orows]))
            waitl(cs)
            if wait_before:
                waits(wait_before)
            base = take(out_tiles) if send_to is not None else None

            def p_copy(t):
                ts = pl.ds(pl.multiple_of(t * tile, tile), tile)
                return rc(dst.at[:, ts], send_to.at[:, ts], 1, base + t)

            @pl.loop(0, out_tiles)
            def _(t):
                ts = pl.ds(pl.multiple_of(t * tile, tile), tile)
                acc = lax.dot_general(hbuf[r], w2v[ts, 0:hid], NT, preferred_element_type=F32)
                acc = acc + lax.dot_general(hr[...], w2v[ts, hid:2 * hid], NT, preferred_element_type=F32)
                acc = acc + lax.dot_general(cbuf[r], w2v[ts, 2 * hid:], TT, preferred_element_type=F32)
                dst[:, ts] = acc
                if send_to is not None:
                    @pl.when(t > 0)
                    def _():
                        p_copy(t - 1).start()
            if send_to is None:
                return []
            p_copy(out_tiles - 1).start()
            return [p_copy(t) for t in range(out_tiles)]

        rest, near = gather0()
        lw = load_first(0)
        res0 = start(lc(x_ref.at[:, pl.ds(ycol, half_d)], nbuf.at[pl.ds(row, seq)]),
                     lc(xg_ref.at[0, 0, pl.ds(orow, seq), pl.ds(ycol, half_d)], nbuf.at[pl.ds(orow, seq)]))
        recvs(lnc)
        waitl(lnl)
        lnf[...] = jnp.zeros_like(lnf)
        for e in range(n):
            lo = ncols * e - 64 * (e % 2)
            lnf[:, lo:lo + win] += lnrec[e].astype(F32)
        wait_prev = {r: [] for r in range(4)}
        p_prev = {'p2': [], 'p31': []}
        for l in range(layers):
            last = l + 1 == layers
            inbound = send_weights(l)
            w_own = own_weights(l)
            w2v[pl.ds(pl.multiple_of(cc * q, 64), cc), 2 * hid:] = wot[q]
            waitl(lw)
            hc, xc = {}, {}
            hc[0], xc[0] = first(l, 0, wait_prev[0], HELD)
            far = rest()
            hc[2], xc[2] = first(l, 2, wait_prev[2], hid_tiles)
            recvs(far)
            hc[3], xc[3] = first(l, 3, wait_prev[3], hid_tiles)
            start(*hc[0][HELD:], xc[0])
            kvs = [kv_send(l, 2, 0), kv_send(l, 3, 0)]
            recvs(near)
            hc[1], xc[1] = first(l, 1, wait_prev[1], hid_tiles)
            kvs += [kv_send(l, r, 1) for r in range(4)] + [kv_send(l, 1, 0)]
            loc = kv_send(l, 0, 0)
            if not last:
                lw = load_first(l + 1)
                lwo = load_out(l + 1)
            w_in = other_weights(l, inbound)
            waitl(w_own)
            waitl(w_in)
            second(l, 2, hc[2], xc[2], p2, None, p_prev['p2'])
            c3 = second(l, 3, hc[3], xc[3], p31, pd3, p_prev['p31'])
            xcs = []
            for t in range(out_tiles):
                ts = slice(t * tile, (t + 1) * tile)
                c3[t].wait_recv()
                p2[:, ts] += pd3[:, ts]
                xcs.append(rc(p2.at[:, tile_cols(t)], px.at[:, tile_cols(t)], 2))
                if t:
                    xcs[t - 1].start()
            xcs[-1].start()
            second(l, 0, hc[0], xc[0], p0, None, [])
            c1 = second(l, 1, hc[1], xc[1], p31, pd1, c3)
            if l == 0:
                waitl(res0)
            waits(sent)
            sent.clear()
            if not last:
                waitl(lwo)
                turn_out()

            def finish(t):
                ts = slice(t * tile, (t + 1) * tile)
                c1[t].wait_recv()
                xcs[t].wait_recv()
                total = p0[:, ts] + pd1[:, ts] + px[:, ts]
                nbuf[:, ts] = (nbuf[:, ts].astype(F32) + total).astype(BF16)

            if not last:
                rest, near = gather1(l + 1, finish)
                wait_prev = {r: hc[r] + [xc[r]] for r in range(4)}
                wait_prev[0] = wait_prev[0] + kvs
                p_prev = {'p2': xcs, 'p31': c1}
                loc.wait()
                kv_in = kvs
            else:
                fin, own = [], []

                def send(t):
                    dc = tile_cols(t, ycol)
                    fin.append(rc(nbuf.at[pl.ds(orow, seq), tile_cols(t)], y_ref.at[:, dc], 4))
                    own.append(lc(nbuf.at[pl.ds(row, seq), tile_cols(t)], y_ref.at[:, dc]))
                    start(fin[t], own[t])
                for t in range(out_tiles):
                    finish(t)
                    if t:
                        send(t - 1)
                send(out_tiles - 1)
                waits(xcs + c1 + [c for r in range(4) for c in hc[r] + [xc[r]]] + kvs + fin)
                recvs(kv_in + kvs + fin)
                waitl(own + [loc])
        waits(lnc)
        assert counter[0] <= cfg['n_remote'] and counter[1] <= cfg['n_local'], counter
    return kernel


def solution(mesh):
    n = mesh.shape['wg']
    batch_spec = P(('dp', 'wg'))
    col_spec = P(None, None, 'wg')
    out_spec = P(None, None, None, 'wg')
    cache_spec = P(None, ('dp', 'wg'))

    def local_program(x, positions, prompt_len, ln_attn, ln_mlp, w_qkv, w_out, w_up, w_down):
        layers, d, _ = w_qkv.shape
        n_heads, hd = w_out.shape[1], w_out.shape[2]
        heads = n_heads // n
        seq, hid, cc = x.shape[1], w_up.shape[2], heads * hd
        two, half_d = 2 * seq, d // 2
        me = lax.axis_index('wg')
        cfg = dict(n=n, layers=layers, seq=seq, d=d, heads=heads, hd=hd, hid=hid, n_remote=192, n_local=96)
        half_hd = hd // 2
        inv_freq = ROPE_BASE ** (-jnp.arange(half_hd, dtype=F32) * 2.0 / hd)
        angles = positions.astype(F32)[None, :] * inv_freq[:, None]
        cos_t, sin_t = (jnp.tile(f(angles), (1, 2)) for f in (jnp.cos, jnp.sin))
        ln = jnp.concatenate([ln_attn, ln_mlp], axis=1).reshape(4 * layers, -1)
        wide = jnp.where(me % 2 == 1, jnp.pad(ln, ((0, 0), (64, 0))), jnp.pad(ln, ((0, 0), (0, 64))))
        win = wide.shape[1]
        lens = jnp.broadcast_to(prompt_len.astype(BF16)[:, None], (1, win))
        ln_piece = jnp.concatenate([wide, lens, jnp.zeros((16 - 4 * layers - 1, win), BF16)], axis=0)
        wq_t = w_qkv.transpose(0, 2, 1)
        wd_t = w_down.transpose(0, 2, 1)
        wo_n = w_out.reshape(layers, d, -1)

        hbm = pl.BlockSpec(memory_space=pltpu.MemorySpace.HBM)
        vmem = pl.BlockSpec(memory_space=pltpu.MemorySpace.VMEM)
        sds = jax.ShapeDtypeStruct
        outs = pl.pallas_call(
            make_kernel(cfg),
            out_shape=[
                sds((seq, d), BF16), sds((layers, 2, d, seq), BF16), sds((layers, 4, two, d), BF16),
                sds((layers, half_d, 2 * hid + 2 * cc), BF16), sds((layers, 4, two, hid), BF16), sds((layers, 4, cc, two), BF16)],
            in_specs=[hbm] * 5 + [hbm, vmem, vmem],
            out_specs=[hbm] * 6,
            scratch_shapes=[
                pltpu.VMEM((3 * cc, d), BF16), pltpu.VMEM((d, hid), BF16), pltpu.VMEM((half_d, 2 * hid + 2 * cc), BF16),
                pltpu.VMEM((d, d // n), BF16), pltpu.VMEM((4, cc, 2 * cc), BF16),
                pltpu.VMEM((two, d), BF16), pltpu.VMEM((two, d), BF16), pltpu.VMEM((two, d), BF16),
                pltpu.VMEM((4, two, hid), BF16), pltpu.VMEM((two, hid), BF16),
                pltpu.VMEM((4, 2, cc, two), BF16), pltpu.VMEM((4, 2 * cc, two), BF16),
                pltpu.VMEM((two, half_d), F32), pltpu.VMEM((two, half_d), F32), pltpu.VMEM((two, half_d), F32),
                pltpu.VMEM((two, half_d), F32), pltpu.VMEM((two, half_d), F32), pltpu.VMEM((two, half_d), F32),
                pltpu.VMEM((two, half_d), BF16), pltpu.VMEM((n, 16, win), BF16), pltpu.VMEM((16, d), F32),
                pltpu.SemaphoreType.DMA((cfg['n_remote'],)), pltpu.SemaphoreType.DMA((cfg['n_remote'],)),
                pltpu.SemaphoreType.DMA((cfg['n_local'],))],
            compiler_params=pltpu.CompilerParams(collective_id=0, has_side_effects=True, vmem_limit_bytes=67043328),
        )(x[0], wq_t, w_up, wd_t, wo_n, ln_piece, cos_t, sin_t)
        y, kv = outs[0], outs[1]
        caches = [kv[:, i].reshape(layers, 1, n_heads, hd, seq).transpose(0, 1, 4, 2, 3) for i in range(2)]
        return y[None], caches[0], caches[1]

    return jax.shard_map(local_program, mesh=mesh, in_specs=(batch_spec, P('dp'), batch_spec, col_spec, col_spec, col_spec, out_spec, col_spec, col_spec), out_specs=(batch_spec, cache_spec, cache_spec), check_vma=False)
```

```python
import jax
import jax.numpy as jnp
from jax import lax
from jax.experimental import pallas as pl
from jax.experimental.pallas import tpu as pltpu
from jax.sharding import PartitionSpec as P

EPSILON = 1e-5
ROPE_BASE = 10000.0
F32 = jnp.float32
BF16 = jnp.bfloat16
MESH = pl.DeviceIdType.MESH
NT = (((1,), (1,)), ((), ()))
TN = (((0,), (0,)), ((), ()))
TT = (((0,), (1,)), ((), ()))
HELD = 3


def flip(v, s):
    if s & 1:
        v = v + 1 - 2 * (v % 2)
    if s & 2:
        v = v + 2 - 4 * ((v // 2) % 2)
    if s & 4:
        v = v + 4 - 8 * ((v // 4) % 2)
    return v


def make_kernel(cfg):
    n, layers, seq, d, heads, hd, hid = (cfg[k] for k in ('n', 'layers', 'seq', 'd', 'heads', 'hd', 'hid'))
    two = 2 * seq
    cc = heads * hd
    half_d = d // 2
    hs = seq // 2
    slot = 3 * hd
    half_hd = hd // 2
    tile = 256
    hid_tiles, out_tiles = hid // tile, half_d // tile
    ncols = d // n
    win = ncols + 64

    def kernel(x_ref, wq_ref, wu_ref, wd_ref, wo_ref, la_ref, lm_ref, len_ref, cos_ref, sin_ref,
               y_ref, k_ref, v_ref, xg_ref, w2_ref, hrec_ref, crec_ref,
               wq, wu, w2v, wob, wot, xbuf, abuf, mbuf, hbuf, hr, kvb, cbuf, p2, p31, p0, pd3, pd1, px, nbuf, lnst, lnsend, lnrec, lnf,
               ssem, rsem, lsem):
        me = lax.axis_index('wg')
        yb = me // 4
        q = me % 4
        row = pl.multiple_of(seq * yb, seq)
        orow = pl.multiple_of(seq * (1 - yb), seq)
        ycol = pl.multiple_of(half_d * yb, half_d)
        ocol = pl.multiple_of(half_d * (1 - yb), half_d)
        counter = [0, 0]

        def take(k=1):
            counter[0] += k
            return counter[0] - k

        def rc(src, dst, s, idx=None):
            i = take() if idx is None else idx
            return pltpu.make_async_remote_copy(src_ref=src, dst_ref=dst, send_sem=ssem.at[i], recv_sem=rsem.at[i],
                                                device_id={'wg': flip(me, s)}, device_id_type=MESH)

        def lc(src, dst):
            counter[1] += 1
            return pltpu.make_async_copy(src, dst, lsem.at[counter[1] - 1])

        def start(*cs):
            for c in cs:
                c.start()
            return cs

        def waits(cs):
            for c in cs:
                c.wait_send()

        def recvs(cs):
            for c in cs:
                c.wait_recv()

        def waitl(cs):
            for c in cs:
                c.wait()

        lnst[...] = jnp.zeros_like(lnst)
        for i in range(layers):
            lnst[4 * i:4 * i + 2, 0:ncols] = la_ref[i].astype(F32)
            lnst[4 * i + 2:4 * i + 4, 0:ncols] = lm_ref[i].astype(F32)
        moved = jnp.where(me % 2 == 1, pltpu.roll(lnst[...], 64, 1), lnst[...])
        is_len = lax.broadcasted_iota(jnp.int32, (16, win), 0) == 4 * layers
        lnsend[...] = jnp.where(is_len, len_ref[0].astype(F32), moved).astype(BF16)
        lnrec[me] = lnsend[...]

        barrier = pltpu.get_barrier_semaphore()
        for s in range(1, n):
            pl.semaphore_signal(barrier, inc=1, device_id={'wg': flip(me, s)}, device_id_type=MESH)
        pl.semaphore_wait(barrier, n - 1)

        sent = []
        lnc = [rc(lnsend, lnrec.at[me], s) for s in range(1, n)]
        start(*lnc)

        def load_out(l):
            return start(lc(wo_ref.at[l], wob))

        def turn_out():
            eye = (lax.broadcasted_iota(jnp.int32, (cc, cc), 0) == lax.broadcasted_iota(jnp.int32, (cc, cc), 1)).astype(F32).astype(BF16)
            for i in range(4):
                pair = jnp.concatenate([wob[cc * i:cc * (i + 1), :], wob[cc * (i + 4):cc * (i + 5), :]], axis=0)
                wot[i] = lax.dot_general(eye, pair, NT, preferred_element_type=F32).astype(BF16)

        def load_first(l):
            return start(lc(wq_ref.at[l], wq), lc(wu_ref.at[l], wu))

        def gather0():
            xt, g = x_ref, xg_ref.at[0]
            y1 = rc(xt.at[pl.ds(0, hs)], g.at[0, pl.ds(row, hs)], 4)
            y2 = rc(xt.at[pl.ds(hs, hs)], g.at[0, pl.ds(row + hs, hs)], 4)
            x1 = rc(xt.at[pl.ds(hs, hs)], g.at[2, pl.ds(row + hs, hs)], 2)
            x2 = rc(xt.at[pl.ds(0, hs)], g.at[2, pl.ds(row, hs)], 2)
            c0 = rc(xt, g.at[1, pl.ds(row, seq)], 1)
            start(y1, x1, y2, x2, c0)
            wl = load_out(0)
            first_weights = load_first(0)
            waitl(wl)
            turn_out()
            y1.wait_recv()
            rx = rc(g.at[0, pl.ds(orow, hs)], g.at[2, pl.ds(orow, hs)], 2)
            rx.start()
            x1.wait_recv()
            ry = rc(g.at[2, pl.ds(row + hs, hs)], g.at[2, pl.ds(row + hs, hs)], 4)
            ry.start()
            y2.wait_recv()
            c1 = rc(g.at[0, pl.ds(orow, seq)], g.at[1, pl.ds(orow, seq)], 1)
            c1.start()
            sent.extend([y1, y2, x1, x2, c0, rx, ry, c1])

            def rest():
                x2.wait_recv()
                c2 = rc(g.at[2, pl.ds(row, seq)], g.at[3, pl.ds(row, seq)], 1)
                c2.start()
                recvs([rx, ry])
                c3 = rc(g.at[2, pl.ds(orow, seq)], g.at[3, pl.ds(orow, seq)], 1)
                c3.start()
                sent.extend([c2, c3])
                return [c2, c3]
            return rest, [c0, c1], first_weights

        def tile_cols(t, base=0):
            off = base + t * tile
            return pl.ds(off if isinstance(off, int) else pl.multiple_of(off, tile), tile)

        def gather1(l, finish):
            g = xg_ref.at[l]
            lo, hi = pl.ds(0, seq), pl.ds(seq, seq)
            ys, xs, own = [], [], []

            def send(t):
                src, dc = nbuf.at[:, tile_cols(t)], tile_cols(t, ycol)
                ys.append(rc(src, g.at[0, :, dc], 4))
                xs.append(rc(src, g.at[2, :, dc], 2))
                own.append(lc(src, g.at[0, :, dc]))
                start(ys[t], xs[t], own[t])
            for t in range(out_tiles):
                finish(t)
                if t:
                    send(t - 1)
            send(out_tiles - 1)
            rx, ry = [], []
            for t in range(out_tiles):
                ys[t].wait_recv()
                oc = tile_cols(t, ocol)
                rx.append(rc(g.at[0, lo, oc], g.at[2, lo, oc], 2))
                rx[t].start()
            waitl(own)
            c1 = rc(g.at[0], g.at[1], 1)
            c1.start()
            for t in range(out_tiles):
                xs[t].wait_recv()
                yc = tile_cols(t, ycol)
                ry.append(rc(g.at[2, hi, yc], g.at[2, hi, yc], 4))
                ry[t].start()
            sent.extend(ys + xs + rx + ry + [c1])

            def rest():
                recvs(rx + ry)
                c3 = rc(g.at[2], g.at[3], 1)
                c3.start()
                sent.append(c3)
                return [c3]
            return rest, [c1]

        def send_weights(l):
            rows = pl.ds(pl.multiple_of(cc * q, 64), cc)
            out = []
            for r in (2, 3, 1):
                t = flip(me, r)
                ty = flip(t, 4)
                out.append(rc(wd_ref.at[l, :, pl.ds(pl.multiple_of(hid * t, 128), hid)], w2_ref.at[l, rows, pl.ds(0, hid)], r))
                out.append(rc(wd_ref.at[l, :, pl.ds(pl.multiple_of(hid * ty, 128), hid)], w2_ref.at[l, rows, pl.ds(hid, hid)], r))
                out.append(rc(wot.at[t % 4], w2_ref.at[l, rows, pl.ds(2 * hid, 2 * cc)], r))
            start(*out)
            sent.extend(out)
            return out

        def own_weights(l):
            rows = pl.ds(pl.multiple_of(cc * q, 64), cc)
            return start(
                lc(wd_ref.at[l, :, pl.ds(pl.multiple_of(hid * me, 128), hid)], w2v.at[rows, pl.ds(0, hid)]),
                lc(wd_ref.at[l, :, pl.ds(pl.multiple_of(hid * flip(me, 4), 128), hid)], w2v.at[rows, pl.ds(hid, hid)]))

        def other_weights(l, inbound):
            recvs(inbound)
            cs = []
            for r in (1, 2, 3):
                rows = pl.ds(pl.multiple_of(cc * flip(q, r), 64), cc)
                cs.append(lc(w2_ref.at[l, rows], w2v.at[rows]))
            return start(*cs)

        def load_x(l, r):
            if l == 0 and r == 0:
                return start(lc(x_ref, xbuf.at[pl.ds(row, seq)]), lc(xg_ref.at[0, 0, pl.ds(orow, seq)], xbuf.at[pl.ds(orow, seq)]))
            return start(lc(xg_ref.at[l, r], xbuf))

        def norm(l):
            @pl.loop(0, two // 16, unroll=4)
            def _(i):
                rs = pl.ds(pl.multiple_of(i * 16, 16), 16)
                v = xbuf[rs, :].astype(F32)
                cen = v - jnp.mean(v, axis=-1, keepdims=True)
                var = jnp.mean(cen * cen, axis=-1, keepdims=True)
                nrm = cen * lax.rsqrt(var + EPSILON)
                k = 4 * l
                abuf[rs, :] = (nrm * lnf[k:k + 1, :] + lnf[k + 1:k + 2, :]).astype(BF16)
                mbuf[rs, :] = (nrm * lnf[k + 2:k + 3, :] + lnf[k + 3:k + 4, :]).astype(BF16)

        def h_copy(l, r, t, base):
            cs = pl.ds(pl.multiple_of(t * tile, tile), tile)
            return rc(hbuf.at[r, :, cs], hrec_ref.at[l, r, :, cs], 4, base + t)

        def up(l, r, base, now):
            @pl.loop(0, hid_tiles)
            def _(t):
                cs = pl.ds(pl.multiple_of(t * tile, tile), tile)
                u = jnp.dot(mbuf[...], wu[:, cs], preferred_element_type=F32)
                hbuf[r, :, cs] = (0.5 * u * (1.0 + lax.erf(u * (0.5 ** 0.5)))).astype(BF16)

                @pl.when((t > 0) & (t <= now))
                def _():
                    h_copy(l, r, t - 1, base).start()
            if now == hid_tiles:
                h_copy(l, r, hid_tiles - 1, base).start()

        def attend(l, r):
            kidx = lax.broadcasted_iota(jnp.int32, (seq, seq), 0)
            qidx = lax.broadcasted_iota(jnp.int32, (seq, seq), 1)
            causal = kidx <= qidx
            kf = kidx.astype(F32)

            @pl.loop(0, heads)
            def _(h):
                t = lax.dot_general(wq[pl.ds(pl.multiple_of(h * slot, 16), slot), :], abuf[...], NT, preferred_element_type=F32)
                t = t.astype(BF16).astype(F32)
                cs, sn = (jnp.concatenate([f[...], f[...]], axis=1) for f in (cos_ref, sin_ref))

                def turn(v):
                    a, b = v[:half_hd], v[half_hd:]
                    return jnp.concatenate([a * cs - b * sn, b * cs + a * sn], axis=0).astype(BF16)
                qr, kr, vr = turn(t[:hd]), turn(t[hd:2 * hd]), t[2 * hd:].astype(BF16)
                hrow = pl.ds(pl.multiple_of(h * hd, 16), hd)
                kvb[r, 0, hrow, :] = kr
                kvb[r, 1, hrow, :] = vr
                crow = pl.ds(pl.multiple_of(cc * yb + h * hd, 16), hd)
                for j in range(2):
                    ps = slice(j * seq, (j + 1) * seq)
                    s = lax.dot_general(kr[:, ps], qr[:, ps], TN, preferred_element_type=F32) * hd ** -0.5
                    plen = lnrec[flip(q, r) + 4 * j, 8:9, 0:seq].astype(F32)
                    s = jnp.where(causal & (kf < plen), s, -1e30)
                    e = jnp.exp(s - jnp.max(s, axis=0, keepdims=True))
                    p = (e / jnp.sum(e, axis=0, keepdims=True)).astype(BF16)
                    cbuf[r, crow, ps] = jnp.dot(vr[:, ps], p, preferred_element_type=F32).astype(BF16)

        def first(l, r, prev, now):
            xs = load_x(l, r)
            if prev:
                waits(prev)
            waitl(xs)
            norm(l)
            base = take(hid_tiles)
            up(l, r, base, now)
            attend(l, r)
            crows = pl.ds(pl.multiple_of(cc * yb, 64), cc)
            c = rc(cbuf.at[r, crows], crec_ref.at[l, r], 4)
            hcs = [h_copy(l, r, t, base) for t in range(hid_tiles)]
            if now == hid_tiles:
                c.start()
            return hcs, c

        def kv_send(l, r, ys):
            j = yb if ys == 0 else 1 - yb
            s = 4 * ys + r
            out = []
            for i, ref in enumerate((k_ref, v_ref)):
                src = kvb.at[r, i, :, pl.ds(pl.multiple_of(seq * j, seq), seq)]
                dst = ref.at[l, pl.ds(pl.multiple_of(cc * me, 64), cc), :]
                out.append(lc(src, dst) if s == 0 else rc(src, dst, s))
            start(*out)
            return out

        def second(l, r, hcs, c, dst, send_to, wait_before):
            recvs(hcs)
            c.wait_recv()
            orows = pl.ds(pl.multiple_of(cc * (1 - yb), 64), cc)
            cs = start(lc(hrec_ref.at[l, r], hr), lc(crec_ref.at[l, r], cbuf.at[r, orows]))
            waitl(cs)
            if wait_before:
                waits(wait_before)
            base = take(out_tiles) if send_to is not None else None

            def p_copy(t):
                ts = pl.ds(pl.multiple_of(t * tile, tile), tile)
                return rc(dst.at[:, ts], send_to.at[:, ts], 1, base + t)

            @pl.loop(0, out_tiles)
            def _(t):
                ts = pl.ds(pl.multiple_of(t * tile, tile), tile)
                acc = lax.dot_general(hbuf[r], w2v[ts, 0:hid], NT, preferred_element_type=F32)
                acc = acc + lax.dot_general(hr[...], w2v[ts, hid:2 * hid], NT, preferred_element_type=F32)
                acc = acc + lax.dot_general(cbuf[r], w2v[ts, 2 * hid:], TT, preferred_element_type=F32)
                dst[:, ts] = acc
                if send_to is not None:
                    @pl.when(t > 0)
                    def _():
                        p_copy(t - 1).start()
            if send_to is None:
                return []
            p_copy(out_tiles - 1).start()
            return [p_copy(t) for t in range(out_tiles)]

        rest, near, lw = gather0()
        res0 = start(lc(x_ref.at[:, pl.ds(ycol, half_d)], nbuf.at[pl.ds(row, seq)]),
                     lc(xg_ref.at[0, 0, pl.ds(orow, seq), pl.ds(ycol, half_d)], nbuf.at[pl.ds(orow, seq)]))
        recvs(lnc)
        lnf[...] = jnp.zeros_like(lnf)
        for e in range(n):
            lo = ncols * e - 64 * (e % 2)
            lnf[:, lo:lo + win] += lnrec[e].astype(F32)
        wait_prev = {r: [] for r in range(4)}
        p_prev = {'p2': [], 'p31': []}
        for l in range(layers):
            last = l + 1 == layers
            inbound = send_weights(l)
            w_own = own_weights(l)
            w2v[pl.ds(pl.multiple_of(cc * q, 64), cc), 2 * hid:] = wot[q]
            waitl(lw)
            hc, xc = {}, {}
            hc[0], xc[0] = first(l, 0, wait_prev[0], HELD)
            far = rest()
            hc[2], xc[2] = first(l, 2, wait_prev[2], hid_tiles)
            recvs(far)
            hc[3], xc[3] = first(l, 3, wait_prev[3], hid_tiles)
            start(*hc[0][HELD:], xc[0])
            kvs = kv_send(l, 2, 0) + kv_send(l, 3, 0) + (kv_send(l, 2, 1) if last else [])
            recvs(near)
            hc[1], xc[1] = first(l, 1, wait_prev[1], hid_tiles)
            for r in range(2 if last else 4):
                kvs += kv_send(l, r, 1)
            kvs += kv_send(l, 1, 0)
            loc = kv_send(l, 0, 0)
            if not last:
                lw = load_first(l + 1)
                lwo = load_out(l + 1)
            w_in = other_weights(l, inbound)
            waitl(w_own)
            waitl(w_in)
            second(l, 2, hc[2], xc[2], p2, None, p_prev['p2'])
            c3 = second(l, 3, hc[3], xc[3], p31, pd3, p_prev['p31'])
            xcs = []
            for t in range(out_tiles):
                ts = slice(t * tile, (t + 1) * tile)
                c3[t].wait_recv()
                p2[:, ts] += pd3[:, ts]
                xcs.append(rc(p2.at[:, tile_cols(t)], px.at[:, tile_cols(t)], 2))
                if t:
                    xcs[t - 1].start()
            xcs[-1].start()
            second(l, 0, hc[0], xc[0], p0, None, [])
            c1 = second(l, 1, hc[1], xc[1], p31, pd1, c3)
            if l == 0:
                waitl(res0)
            waits(sent)
            sent.clear()
            if not last:
                waitl(lwo)
                turn_out()

            def finish(t):
                ts = slice(t * tile, (t + 1) * tile)
                c1[t].wait_recv()
                xcs[t].wait_recv()
                total = p0[:, ts] + pd1[:, ts] + px[:, ts]
                nbuf[:, ts] = (nbuf[:, ts].astype(F32) + total).astype(BF16)

            if not last:
                rest, near = gather1(l + 1, finish)
                wait_prev = {r: hc[r] + [xc[r]] for r in range(4)}
                wait_prev[0] = wait_prev[0] + kvs
                p_prev = {'p2': xcs, 'p31': c1}
                waitl(loc)
                kv_in = kvs
            else:
                fin, own = [], []

                def send(t):
                    dc = tile_cols(t, ycol)
                    fin.append(rc(nbuf.at[pl.ds(orow, seq), tile_cols(t)], y_ref.at[:, dc], 4))
                    own.append(lc(nbuf.at[pl.ds(row, seq), tile_cols(t)], y_ref.at[:, dc]))
                    start(fin[t], own[t])
                for t in range(out_tiles):
                    finish(t)
                    if t:
                        send(t - 1)
                send(out_tiles - 1)
                kvs += kv_send(l, 3, 1)
                waits(xcs + c1 + [c for r in range(4) for c in hc[r] + [xc[r]]] + kvs + fin)
                recvs(kv_in + kvs + fin)
                waitl(own + loc)
        waits(lnc)
        assert counter[0] <= cfg['n_remote'] and counter[1] <= cfg['n_local'], counter
    return kernel


def solution(mesh):
    n = mesh.shape['wg']
    batch_spec = P(('dp', 'wg'))
    col_spec = P(None, None, 'wg')
    out_spec = P(None, None, None, 'wg')
    cache_spec = P(None, ('dp', 'wg'))

    def local_program(x, positions, prompt_len, ln_attn, ln_mlp, w_qkv, w_out, w_up, w_down):
        layers, d, _ = w_qkv.shape
        n_heads, hd = w_out.shape[1], w_out.shape[2]
        heads = n_heads // n
        seq, hid, cc = x.shape[1], w_up.shape[2], heads * hd
        two, half_d = 2 * seq, d // 2
        me = lax.axis_index('wg')
        cfg = dict(n=n, layers=layers, seq=seq, d=d, heads=heads, hd=hd, hid=hid, n_remote=192, n_local=96)
        half_hd = hd // 2
        inv_freq = ROPE_BASE ** (-jnp.arange(half_hd, dtype=F32) * 2.0 / hd)
        angles = positions.astype(F32)[None, :] * inv_freq[:, None]
        cos_t, sin_t = jnp.cos(angles), jnp.sin(angles)
        win = d // n + 64
        wq_t = w_qkv.transpose(0, 2, 1)
        wd_t = w_down.transpose(0, 2, 1)
        wo_n = w_out.reshape(layers, d, -1)

        hbm = pl.BlockSpec(memory_space=pltpu.MemorySpace.HBM)
        vmem = pl.BlockSpec(memory_space=pltpu.MemorySpace.VMEM)
        sds = jax.ShapeDtypeStruct
        outs = pl.pallas_call(
            make_kernel(cfg),
            out_shape=[
                sds((seq, d), BF16), sds((layers, d, seq), BF16), sds((layers, d, seq), BF16), sds((layers, 4, two, d), BF16),
                sds((layers, half_d, 2 * hid + 2 * cc), BF16), sds((layers, 4, two, hid), BF16), sds((layers, 4, cc, two), BF16)],
            in_specs=[hbm] * 5 + [vmem, vmem, pl.BlockSpec(memory_space=pltpu.MemorySpace.SMEM), vmem, vmem],
            out_specs=[hbm] * 7,
            scratch_shapes=[
                pltpu.VMEM((3 * cc, d), BF16), pltpu.VMEM((d, hid), BF16), pltpu.VMEM((half_d, 2 * hid + 2 * cc), BF16),
                pltpu.VMEM((d, d // n), BF16), pltpu.VMEM((4, cc, 2 * cc), BF16),
                pltpu.VMEM((two, d), BF16), pltpu.VMEM((two, d), BF16), pltpu.VMEM((two, d), BF16),
                pltpu.VMEM((4, two, hid), BF16), pltpu.VMEM((two, hid), BF16),
                pltpu.VMEM((4, 2, cc, two), BF16), pltpu.VMEM((4, 2 * cc, two), BF16),
                pltpu.VMEM((two, half_d), F32), pltpu.VMEM((two, half_d), F32), pltpu.VMEM((two, half_d), F32),
                pltpu.VMEM((two, half_d), F32), pltpu.VMEM((two, half_d), F32), pltpu.VMEM((two, half_d), F32),
                pltpu.VMEM((two, half_d), BF16), pltpu.VMEM((16, win), F32), pltpu.VMEM((16, win), BF16), pltpu.VMEM((n, 16, win), BF16), pltpu.VMEM((16, d), F32),
                pltpu.SemaphoreType.DMA((cfg['n_remote'],)), pltpu.SemaphoreType.DMA((cfg['n_remote'],)),
                pltpu.SemaphoreType.DMA((cfg['n_local'],))],
            compiler_params=pltpu.CompilerParams(collective_id=0, has_side_effects=True, vmem_limit_bytes=67043328),
        )(x[0], wq_t, w_up, wd_t, wo_n, ln_attn, ln_mlp, prompt_len, cos_t, sin_t)
        caches = [c.reshape(layers, 1, n_heads, hd, seq).transpose(0, 1, 4, 2, 3) for c in outs[1:3]]
        return outs[0][None], caches[0], caches[1]

    return jax.shard_map(local_program, mesh=mesh, in_specs=(batch_spec, P('dp'), batch_spec, col_spec, col_spec, col_spec, out_spec, col_spec, col_spec), out_specs=(batch_spec, cache_spec, cache_spec), check_vma=False)
```

```python
import jax
import jax.numpy as jnp
import numpy as np
from jax import lax
from jax.experimental import pallas as pl
from jax.experimental.pallas import tpu as pltpu
from jax.sharding import PartitionSpec as P

EPSILON = 1e-5
ROPE_BASE = 10000.0
F32 = jnp.float32
BF16 = jnp.bfloat16
MESH = pl.DeviceIdType.MESH
NT = (((1,), (1,)), ((), ()))
TN = (((0,), (0,)), ((), ()))
TT = (((0,), (1,)), ((), ()))
HELD = 3


def flip(v, s):
    if s & 1:
        v = v + 1 - 2 * (v % 2)
    if s & 2:
        v = v + 2 - 4 * ((v // 2) % 2)
    if s & 4:
        v = v + 4 - 8 * ((v // 4) % 2)
    return v


def make_kernel(cfg):
    n, layers, seq, d, heads, hd, hid = (cfg[k] for k in ('n', 'layers', 'seq', 'd', 'heads', 'hd', 'hid'))
    two = 2 * seq
    cc = heads * hd
    half_d = d // 2
    hs = 112
    ht = seq - hs
    slot = 3 * hd
    half_hd = hd // 2
    tile = 256
    hid_tiles, out_tiles = hid // tile, half_d // tile
    ncols = d // n
    win = ncols + 64

    def kernel(x_ref, wq_ref, wu_ref, wd_ref, wo_ref, la_ref, lm_ref, len_ref, pos_ref, freq_ref,
               y_ref, k_ref, v_ref, xg_ref, w2_ref, hrec_ref, crec_ref,
               wq, wu, w2v, wob, wot, xbuf, abuf, mbuf, hbuf, hr, kvb, cbuf, p2, p31, p0, pd3, pd1, px, nbuf, cos_ref, sin_ref, lnst, lnsend, lnrec, lnf,
               ssem, rsem, lsem):
        me = lax.axis_index('wg')
        yb = me // 4
        q = me % 4
        row = pl.multiple_of(seq * yb, seq)
        orow = pl.multiple_of(seq * (1 - yb), seq)
        ycol = pl.multiple_of(half_d * yb, half_d)
        ocol = pl.multiple_of(half_d * (1 - yb), half_d)
        counter = [0, 0]

        def take(k=1):
            counter[0] += k
            return counter[0] - k

        def rc(src, dst, s, idx=None):
            i = take() if idx is None else idx
            return pltpu.make_async_remote_copy(src_ref=src, dst_ref=dst, send_sem=ssem.at[i], recv_sem=rsem.at[i],
                                                device_id={'wg': flip(me, s)}, device_id_type=MESH)

        def lc(src, dst):
            counter[1] += 1
            return pltpu.make_async_copy(src, dst, lsem.at[counter[1] - 1])

        def start(*cs):
            for c in cs:
                c.start()
            return cs

        def waits(cs):
            for c in cs:
                c.wait_send()

        def recvs(cs):
            for c in cs:
                c.wait_recv()

        def waitl(cs):
            for c in cs:
                c.wait()

        barrier = pltpu.get_barrier_semaphore()
        for s in range(1, n):
            pl.semaphore_signal(barrier, inc=1, device_id={'wg': flip(me, s)}, device_id_type=MESH)

        angles = freq_ref[...] * pos_ref[...].astype(F32)
        for f, ref in ((jnp.cos, cos_ref), (jnp.sin, sin_ref)):
            ref[:, 0:seq] = f(angles)
            ref[:, seq:two] = ref[:, 0:seq]

        lnst[...] = jnp.zeros_like(lnst)
        for i in range(layers):
            lnst[4 * i:4 * i + 2, 0:ncols] = la_ref[i].astype(F32)
            lnst[4 * i + 2:4 * i + 4, 0:ncols] = lm_ref[i].astype(F32)
        moved = jnp.where(me % 2 == 1, pltpu.roll(lnst[...], 64, 1), lnst[...])
        is_len = lax.broadcasted_iota(jnp.int32, (16, win), 0) == 4 * layers
        lnsend[...] = jnp.where(is_len, len_ref[0].astype(F32), moved).astype(BF16)
        lnrec[me] = lnsend[...]
        pl.semaphore_wait(barrier, n - 1)

        sent = []
        lnc = [rc(lnsend, lnrec.at[me], s) for s in range(1, n)]

        def load_out(l):
            return start(lc(wo_ref.at[l], wob))

        def turn_out():
            eye = (lax.broadcasted_iota(jnp.int32, (cc, cc), 0) == lax.broadcasted_iota(jnp.int32, (cc, cc), 1)).astype(F32).astype(BF16)
            for i in range(4):
                pair = jnp.concatenate([wob[cc * i:cc * (i + 1), :], wob[cc * (i + 4):cc * (i + 5), :]], axis=0)
                wot[i] = lax.dot_general(eye, pair, NT, preferred_element_type=F32).astype(BF16)

        def load_first(l):
            return start(lc(wq_ref.at[l], wq), lc(wu_ref.at[l], wu))

        def gather0():
            xt, g = x_ref, xg_ref.at[0]
            y1 = rc(xt.at[pl.ds(0, hs)], g.at[0, pl.ds(row, hs)], 4)
            y2 = rc(xt.at[pl.ds(hs, ht)], g.at[0, pl.ds(row + hs, ht)], 4)
            x1 = rc(xt.at[pl.ds(hs, ht)], g.at[2, pl.ds(row + hs, ht)], 2)
            x2 = rc(xt.at[pl.ds(0, hs)], g.at[2, pl.ds(row, hs)], 2)
            c0 = rc(xt, g.at[1, pl.ds(row, seq)], 1)
            start(y1, x1, y2, x2, c0, *lnc)
            wl = load_out(0)
            first_weights = load_first(0)
            waitl(wl)
            turn_out()
            y1.wait_recv()
            rx = rc(g.at[0, pl.ds(orow, hs)], g.at[2, pl.ds(orow, hs)], 2)
            rx.start()
            x1.wait_recv()
            ry = rc(g.at[2, pl.ds(row + hs, ht)], g.at[2, pl.ds(row + hs, ht)], 4)
            ry.start()
            y2.wait_recv()
            c1 = rc(g.at[0, pl.ds(orow, seq)], g.at[1, pl.ds(orow, seq)], 1)
            c1.start()
            sent.extend([y1, y2, x1, x2, c0, rx, ry, c1])

            def rest():
                x2.wait_recv()
                c2 = rc(g.at[2, pl.ds(row, seq)], g.at[3, pl.ds(row, seq)], 1)
                c2.start()
                recvs([rx, ry])
                c3 = rc(g.at[2, pl.ds(orow, seq)], g.at[3, pl.ds(orow, seq)], 1)
                c3.start()
                sent.extend([c2, c3])
                return [c2, c3]
            return rest, [c0, c1], first_weights

        def tile_cols(t, base=0):
            off = base + t * tile
            return pl.ds(off if isinstance(off, int) else pl.multiple_of(off, tile), tile)

        def gather1(l, finish):
            g = xg_ref.at[l]
            lo, hi = pl.ds(0, 304), pl.ds(304, two - 304)
            ys, xs, own = [], [], []

            def send(t):
                src, dc = nbuf.at[:, tile_cols(t)], tile_cols(t, ycol)
                ys.append(rc(src, g.at[0, :, dc], 4))
                xs.append(rc(src, g.at[2, :, dc], 2))
                own.append(lc(src, g.at[0, :, dc]))
                start(ys[t], xs[t], own[t])
            for t in range(out_tiles):
                finish(t)
                if t:
                    send(t - 1)
            send(out_tiles - 1)
            rx, ry = [], []
            for t in range(out_tiles):
                ys[t].wait_recv()
                oc = tile_cols(t, ocol)
                rx.append(rc(g.at[0, lo, oc], g.at[2, lo, oc], 2))
                rx[t].start()
            waitl(own)
            c1 = rc(g.at[0], g.at[1], 1)
            c1.start()
            for t in range(out_tiles):
                xs[t].wait_recv()
                yc = tile_cols(t, ycol)
                ry.append(rc(g.at[2, hi, yc], g.at[2, hi, yc], 4))
                ry[t].start()
            sent.extend(ys + xs + rx + ry + [c1])

            def rest():
                recvs(rx + ry)
                c3 = rc(g.at[2], g.at[3], 1)
                c3.start()
                sent.append(c3)
                return [c3]
            return rest, [c1]

        def send_weights(l):
            rows = pl.ds(pl.multiple_of(cc * q, 64), cc)
            out = []
            for r in (2, 3, 1):
                t = flip(me, r)
                ty = flip(t, 4)
                out.append(rc(wd_ref.at[l, :, pl.ds(pl.multiple_of(hid * t, 128), hid)], w2_ref.at[l, rows, pl.ds(0, hid)], r))
                out.append(rc(wd_ref.at[l, :, pl.ds(pl.multiple_of(hid * ty, 128), hid)], w2_ref.at[l, rows, pl.ds(hid, hid)], r))
                out.append(rc(wot.at[t % 4], w2_ref.at[l, rows, pl.ds(2 * hid, 2 * cc)], r))
            start(*out)
            sent.extend(out)
            return out

        def own_weights(l):
            rows = pl.ds(pl.multiple_of(cc * q, 64), cc)
            return start(
                lc(wd_ref.at[l, :, pl.ds(pl.multiple_of(hid * me, 128), hid)], w2v.at[rows, pl.ds(0, hid)]),
                lc(wd_ref.at[l, :, pl.ds(pl.multiple_of(hid * flip(me, 4), 128), hid)], w2v.at[rows, pl.ds(hid, hid)]))

        def other_weights(l, inbound):
            recvs(inbound)
            cs = []
            for r in (1, 2, 3):
                rows = pl.ds(pl.multiple_of(cc * flip(q, r), 64), cc)
                cs.append(lc(w2_ref.at[l, rows], w2v.at[rows]))
            return start(*cs)

        def load_x(l, r):
            if l == 0 and r == 0:
                return start(lc(x_ref, xbuf.at[pl.ds(row, seq)]), lc(xg_ref.at[0, 0, pl.ds(orow, seq)], xbuf.at[pl.ds(orow, seq)]))
            return start(lc(xg_ref.at[l, r], xbuf))

        def norm(l):
            @pl.loop(0, two // 16, unroll=4)
            def _(i):
                rs = pl.ds(pl.multiple_of(i * 16, 16), 16)
                v = xbuf[rs, :].astype(F32)
                cen = v - jnp.mean(v, axis=-1, keepdims=True)
                var = jnp.mean(cen * cen, axis=-1, keepdims=True)
                nrm = cen * lax.rsqrt(var + EPSILON)
                k = 4 * l
                abuf[rs, :] = (nrm * lnf[k:k + 1, :] + lnf[k + 1:k + 2, :]).astype(BF16)
                mbuf[rs, :] = (nrm * lnf[k + 2:k + 3, :] + lnf[k + 3:k + 4, :]).astype(BF16)

        def h_copy(l, r, t, base):
            cs = pl.ds(pl.multiple_of(t * tile, tile), tile)
            return rc(hbuf.at[r, :, cs], hrec_ref.at[l, r, :, cs], 4, base + t)

        def up(l, r, base, now):
            @pl.loop(0, hid_tiles)
            def _(t):
                cs = pl.ds(pl.multiple_of(t * tile, tile), tile)
                u = jnp.dot(mbuf[...], wu[:, cs], preferred_element_type=F32)
                hbuf[r, :, cs] = (0.5 * u * (1.0 + lax.erf(u * (0.5 ** 0.5)))).astype(BF16)

                @pl.when((t > 0) & (t <= now))
                def _():
                    h_copy(l, r, t - 1, base).start()
            if now == hid_tiles:
                h_copy(l, r, hid_tiles - 1, base).start()

        def attend(l, r):
            kidx = lax.broadcasted_iota(jnp.int32, (seq, seq), 0)
            qidx = lax.broadcasted_iota(jnp.int32, (seq, seq), 1)
            causal = kidx <= qidx
            kf = kidx.astype(F32)

            @pl.loop(0, heads)
            def _(h):
                t = lax.dot_general(wq[pl.ds(pl.multiple_of(h * slot, 16), slot), :], abuf[...], NT, preferred_element_type=F32)
                t = t.astype(BF16).astype(F32)
                cs, sn = cos_ref[...], sin_ref[...]

                def turn(v):
                    a, b = v[:half_hd], v[half_hd:]
                    return jnp.concatenate([a * cs - b * sn, b * cs + a * sn], axis=0).astype(BF16)
                qr, kr, vr = turn(t[:hd]), turn(t[hd:2 * hd]), t[2 * hd:].astype(BF16)
                hrow = pl.ds(pl.multiple_of(h * hd, 16), hd)
                kvb[r, 0, hrow, :] = kr
                kvb[r, 1, hrow, :] = vr
                crow = pl.ds(pl.multiple_of(cc * yb + h * hd, 16), hd)
                for j in range(2):
                    ps = slice(j * seq, (j + 1) * seq)
                    s = lax.dot_general(kr[:, ps], qr[:, ps], TN, preferred_element_type=F32) * hd ** -0.5
                    plen = lnrec[flip(q, r) + 4 * j, 8:9, 0:seq].astype(F32)
                    s = jnp.where(causal & (kf < plen), s, -1e30)
                    e = jnp.exp(s - jnp.max(s, axis=0, keepdims=True))
                    p = (e / jnp.sum(e, axis=0, keepdims=True)).astype(BF16)
                    cbuf[r, crow, ps] = jnp.dot(vr[:, ps], p, preferred_element_type=F32).astype(BF16)

        def first(l, r, prev, now):
            xs = load_x(l, r)
            if prev:
                waits(prev)
            waitl(xs)
            norm(l)
            base = take(hid_tiles)
            up(l, r, base, now)
            attend(l, r)
            crows = pl.ds(pl.multiple_of(cc * yb, 64), cc)
            c = rc(cbuf.at[r, crows], crec_ref.at[l, r], 4)
            hcs = [h_copy(l, r, t, base) for t in range(hid_tiles)]
            if now == hid_tiles:
                c.start()
            return hcs, c

        def kv_send(l, r, ys):
            j = yb if ys == 0 else 1 - yb
            s = 4 * ys + r
            out = []
            for i, ref in enumerate((k_ref, v_ref)):
                src = kvb.at[r, i, :, pl.ds(pl.multiple_of(seq * j, seq), seq)]
                dst = ref.at[l, pl.ds(pl.multiple_of(cc * me, 64), cc), :]
                out.append(lc(src, dst) if s == 0 else rc(src, dst, s))
            start(*out)
            return out

        def second(l, r, hcs, c, dst, send_to, wait_before):
            recvs(hcs)
            c.wait_recv()
            orows = pl.ds(pl.multiple_of(cc * (1 - yb), 64), cc)
            cs = start(lc(hrec_ref.at[l, r], hr), lc(crec_ref.at[l, r], cbuf.at[r, orows]))
            waitl(cs)
            if wait_before:
                waits(wait_before)
            base = take(out_tiles) if send_to is not None else None

            def p_copy(t):
                ts = pl.ds(pl.multiple_of(t * tile, tile), tile)
                return rc(dst.at[:, ts], send_to.at[:, ts], 1, base + t)

            @pl.loop(0, out_tiles)
            def _(t):
                ts = pl.ds(pl.multiple_of(t * tile, tile), tile)
                acc = lax.dot_general(hbuf[r], w2v[ts, 0:hid], NT, preferred_element_type=F32)
                acc = acc + lax.dot_general(hr[...], w2v[ts, hid:2 * hid], NT, preferred_element_type=F32)
                acc = acc + lax.dot_general(cbuf[r], w2v[ts, 2 * hid:], TT, preferred_element_type=F32)
                dst[:, ts] = acc
                if send_to is not None:
                    @pl.when(t > 0)
                    def _():
                        p_copy(t - 1).start()
            if send_to is None:
                return []
            p_copy(out_tiles - 1).start()
            return [p_copy(t) for t in range(out_tiles)]

        rest, near, lw = gather0()
        res0 = start(lc(x_ref.at[:, pl.ds(ycol, half_d)], nbuf.at[pl.ds(row, seq)]),
                     lc(xg_ref.at[0, 0, pl.ds(orow, seq), pl.ds(ycol, half_d)], nbuf.at[pl.ds(orow, seq)]))
        recvs(lnc)
        lnf[...] = jnp.zeros_like(lnf)
        for e in range(n):
            lo = ncols * e - 64 * (e % 2)
            lnf[:, lo:lo + win] += lnrec[e].astype(F32)
        wait_prev = {r: [] for r in range(4)}
        p_prev = {'p2': [], 'p31': []}
        for l in range(layers):
            last = l + 1 == layers
            inbound = send_weights(l)
            w_own = own_weights(l)
            w2v[pl.ds(pl.multiple_of(cc * q, 64), cc), 2 * hid:] = wot[q]
            waitl(lw)
            hc, xc = {}, {}
            hc[0], xc[0] = first(l, 0, wait_prev[0], HELD)
            far = rest()
            hc[2], xc[2] = first(l, 2, wait_prev[2], hid_tiles)
            recvs(far)
            hc[3], xc[3] = first(l, 3, wait_prev[3], hid_tiles)
            start(*hc[0][HELD:], xc[0])
            kvs = kv_send(l, 2, 0) + kv_send(l, 3, 0) + (kv_send(l, 2, 1) if last else [])
            recvs(near)
            hc[1], xc[1] = first(l, 1, wait_prev[1], hid_tiles)
            for r in range(2 if last else 4):
                kvs += kv_send(l, r, 1)
            kvs += kv_send(l, 1, 0)
            loc = kv_send(l, 0, 0)
            if not last:
                lw = load_first(l + 1)
                lwo = load_out(l + 1)
            w_in = other_weights(l, inbound)
            waitl(w_own)
            waitl(w_in)
            second(l, 2, hc[2], xc[2], p2, None, p_prev['p2'])
            c3 = second(l, 3, hc[3], xc[3], p31, pd3, p_prev['p31'])
            xcs = []
            for t in range(out_tiles):
                ts = slice(t * tile, (t + 1) * tile)
                c3[t].wait_recv()
                p2[:, ts] += pd3[:, ts]
                xcs.append(rc(p2.at[:, tile_cols(t)], px.at[:, tile_cols(t)], 2))
                if t:
                    xcs[t - 1].start()
            xcs[-1].start()
            second(l, 0, hc[0], xc[0], p0, None, [])
            c1 = second(l, 1, hc[1], xc[1], p31, pd1, c3)
            if l == 0:
                waitl(res0)
            waits(sent)
            sent.clear()
            if not last:
                waitl(lwo)
                turn_out()

            def finish(t):
                ts = slice(t * tile, (t + 1) * tile)
                c1[t].wait_recv()
                xcs[t].wait_recv()
                total = p0[:, ts] + pd1[:, ts] + px[:, ts]
                nbuf[:, ts] = (nbuf[:, ts].astype(F32) + total).astype(BF16)

            if not last:
                rest, near = gather1(l + 1, finish)
                wait_prev = {r: hc[r] + [xc[r]] for r in range(4)}
                wait_prev[0] = wait_prev[0] + kvs
                p_prev = {'p2': xcs, 'p31': c1}
                waitl(loc)
                kv_in = kvs
            else:
                fin, own = [], []

                def send(t):
                    dc = tile_cols(t, ycol)
                    fin.append(rc(nbuf.at[pl.ds(orow, seq), tile_cols(t)], y_ref.at[:, dc], 4))
                    own.append(lc(nbuf.at[pl.ds(row, seq), tile_cols(t)], y_ref.at[:, dc]))
                    start(fin[t], own[t])
                for t in range(out_tiles):
                    finish(t)
                    if t:
                        send(t - 1)
                send(out_tiles - 1)
                kvs += kv_send(l, 3, 1)
                waits(xcs + c1 + [c for r in range(4) for c in hc[r] + [xc[r]]] + kvs + fin)
                recvs(kv_in + kvs + fin)
                waitl(own + loc)
        waits(lnc)
        assert counter[0] <= cfg['n_remote'] and counter[1] <= cfg['n_local'], counter
    return kernel


def solution(mesh):
    n = mesh.shape['wg']
    batch_spec = P(('dp', 'wg'))
    col_spec = P(None, None, 'wg')
    out_spec = P(None, None, None, 'wg')
    cache_spec = P(None, ('dp', 'wg'))

    def local_program(x, positions, prompt_len, ln_attn, ln_mlp, w_qkv, w_out, w_up, w_down):
        layers, d, _ = w_qkv.shape
        n_heads, hd = w_out.shape[1], w_out.shape[2]
        heads = n_heads // n
        seq, hid, cc = x.shape[1], w_up.shape[2], heads * hd
        two, half_d = 2 * seq, d // 2
        me = lax.axis_index('wg')
        cfg = dict(n=n, layers=layers, seq=seq, d=d, heads=heads, hd=hd, hid=hid, n_remote=192, n_local=96)
        half_hd = hd // 2
        inv_freq = (ROPE_BASE ** (-np.arange(half_hd) * 2.0 / hd)).astype(np.float32)
        freq = jnp.asarray(inv_freq[:, None])
        win = d // n + 64
        wq_t = w_qkv.transpose(0, 2, 1)
        wd_t = w_down.transpose(0, 2, 1)
        wo_n = w_out.reshape(layers, d, -1)

        hbm = pl.BlockSpec(memory_space=pltpu.MemorySpace.HBM)
        vmem = pl.BlockSpec(memory_space=pltpu.MemorySpace.VMEM)
        sds = jax.ShapeDtypeStruct
        outs = pl.pallas_call(
            make_kernel(cfg),
            out_shape=[
                sds((seq, d), BF16), sds((layers, d, seq), BF16), sds((layers, d, seq), BF16), sds((layers, 4, two, d), BF16),
                sds((layers, half_d, 2 * hid + 2 * cc), BF16), sds((layers, 4, two, hid), BF16), sds((layers, 4, cc, two), BF16)],
            in_specs=[hbm] * 5 + [vmem, vmem, pl.BlockSpec(memory_space=pltpu.MemorySpace.SMEM), vmem, vmem],
            out_specs=[hbm] * 7,
            scratch_shapes=[
                pltpu.VMEM((3 * cc, d), BF16), pltpu.VMEM((d, hid), BF16), pltpu.VMEM((half_d, 2 * hid + 2 * cc), BF16),
                pltpu.VMEM((d, d // n), BF16), pltpu.VMEM((4, cc, 2 * cc), BF16),
                pltpu.VMEM((two, d), BF16), pltpu.VMEM((two, d), BF16), pltpu.VMEM((two, d), BF16),
                pltpu.VMEM((4, two, hid), BF16), pltpu.VMEM((two, hid), BF16),
                pltpu.VMEM((4, 2, cc, two), BF16), pltpu.VMEM((4, 2 * cc, two), BF16),
                pltpu.VMEM((two, half_d), F32), pltpu.VMEM((two, half_d), F32), pltpu.VMEM((two, half_d), F32),
                pltpu.VMEM((two, half_d), F32), pltpu.VMEM((two, half_d), F32), pltpu.VMEM((two, half_d), F32),
                pltpu.VMEM((two, half_d), BF16), pltpu.VMEM((half_hd, two), F32), pltpu.VMEM((half_hd, two), F32), pltpu.VMEM((16, win), F32), pltpu.VMEM((16, win), BF16), pltpu.VMEM((n, 16, win), BF16), pltpu.VMEM((16, d), F32),
                pltpu.SemaphoreType.DMA((cfg['n_remote'],)), pltpu.SemaphoreType.DMA((cfg['n_remote'],)),
                pltpu.SemaphoreType.DMA((cfg['n_local'],))],
            compiler_params=pltpu.CompilerParams(collective_id=0, has_side_effects=True, vmem_limit_bytes=67043328),
        )(x[0], wq_t, w_up, wd_t, wo_n, ln_attn, ln_mlp, prompt_len, positions[None, :], freq)
        caches = [c.reshape(layers, 1, n_heads, hd, seq).transpose(0, 1, 4, 2, 3) for c in outs[1:3]]
        return outs[0][None], caches[0], caches[1]

    return jax.shard_map(local_program, mesh=mesh, in_specs=(batch_spec, P('dp'), batch_spec, col_spec, col_spec, col_spec, out_spec, col_spec, col_spec), out_specs=(batch_spec, cache_spec, cache_spec), check_vma=False)
```

```python
import jax
import jax.numpy as jnp
import numpy as np
from jax import lax
from jax.experimental import pallas as pl
from jax.experimental.pallas import tpu as pltpu
from jax.sharding import PartitionSpec as P

EPSILON = 1e-5
ROPE_BASE = 10000.0
F32 = jnp.float32
BF16 = jnp.bfloat16
MESH = pl.DeviceIdType.MESH
NT = (((1,), (1,)), ((), ()))
TN = (((0,), (0,)), ((), ()))
TT = (((0,), (1,)), ((), ()))
HELD = 3


def flip(v, s):
    if s & 1:
        v = v + 1 - 2 * (v % 2)
    if s & 2:
        v = v + 2 - 4 * ((v // 2) % 2)
    if s & 4:
        v = v + 4 - 8 * ((v // 4) % 2)
    return v


def make_kernel(cfg):
    n, layers, seq, d, heads, hd, hid = (cfg[k] for k in ('n', 'layers', 'seq', 'd', 'heads', 'hd', 'hid'))
    two = 2 * seq
    cc = heads * hd
    half_d = d // 2
    hs = 112
    ht = seq - hs
    slot = 3 * hd
    half_hd = hd // 2
    tile = 256
    hid_tiles, out_tiles = hid // tile, half_d // tile
    ncols = d // n
    win = ncols + 64

    def kernel(x_ref, wq_ref, wu_ref, wd_ref, wo_ref, la_ref, lm_ref, len_ref, pos_ref, freq_ref,
               y_ref, k_ref, v_ref, xg_ref, w2_ref, hrec_ref, crec_ref,
               wq, wu, w2v, wob, wot, xbuf, abuf, mbuf, hbuf, hr, kvb, cbuf, p2, p31, p0, pd3, pd1, px, nbuf, cos_ref, sin_ref, lnst, lnsend, lnrec, lnf,
               ssem, rsem, lsem):
        me = lax.axis_index('wg')
        yb = me // 4
        q = me % 4
        row = pl.multiple_of(seq * yb, seq)
        orow = pl.multiple_of(seq * (1 - yb), seq)
        ycol = pl.multiple_of(half_d * yb, half_d)
        ocol = pl.multiple_of(half_d * (1 - yb), half_d)
        counter = [0, 0]

        def take(k=1):
            counter[0] += k
            return counter[0] - k

        def rc(src, dst, s, idx=None):
            i = take() if idx is None else idx
            return pltpu.make_async_remote_copy(src_ref=src, dst_ref=dst, send_sem=ssem.at[i], recv_sem=rsem.at[i],
                                                device_id={'wg': flip(me, s)}, device_id_type=MESH)

        def lc(src, dst):
            counter[1] += 1
            return pltpu.make_async_copy(src, dst, lsem.at[counter[1] - 1])

        def start(*cs):
            for c in cs:
                c.start()
            return cs

        def waits(cs):
            for c in cs:
                c.wait_send()

        def recvs(cs):
            for c in cs:
                c.wait_recv()

        def waitl(cs):
            for c in cs:
                c.wait()

        barrier = pltpu.get_barrier_semaphore()
        for s in range(1, n):
            pl.semaphore_signal(barrier, inc=1, device_id={'wg': flip(me, s)}, device_id_type=MESH)

        angles = freq_ref[...] * pos_ref[...].astype(F32)
        for f, ref in ((jnp.cos, cos_ref), (jnp.sin, sin_ref)):
            ref[:, 0:seq] = f(angles)
            ref[:, seq:two] = ref[:, 0:seq]

        lnst[...] = jnp.zeros_like(lnst)
        for i in range(layers):
            lnst[4 * i:4 * i + 2, 0:ncols] = la_ref[i].astype(F32)
            lnst[4 * i + 2:4 * i + 4, 0:ncols] = lm_ref[i].astype(F32)
        moved = jnp.where(me % 2 == 1, pltpu.roll(lnst[...], 64, 1), lnst[...])
        is_len = lax.broadcasted_iota(jnp.int32, (16, win), 0) == 4 * layers
        lnsend[...] = jnp.where(is_len, len_ref[0].astype(F32), moved).astype(BF16)
        lnrec[me] = lnsend[...]
        pl.semaphore_wait(barrier, n - 1)

        sent = []
        lnc = [rc(lnsend, lnrec.at[me], s) for s in range(1, n)]

        def load_out(l):
            return start(lc(wo_ref.at[l], wob))

        def turn_out():
            eye = (lax.broadcasted_iota(jnp.int32, (cc, cc), 0) == lax.broadcasted_iota(jnp.int32, (cc, cc), 1)).astype(F32).astype(BF16)
            for i in range(4):
                pair = jnp.concatenate([wob[cc * i:cc * (i + 1), :], wob[cc * (i + 4):cc * (i + 5), :]], axis=0)
                wot[i] = lax.dot_general(eye, pair, NT, preferred_element_type=F32).astype(BF16)

        def load_first(l):
            return start(lc(wq_ref.at[l], wq), lc(wu_ref.at[l], wu))

        def gather0():
            xt, g = x_ref, xg_ref.at[0]
            y1 = rc(xt.at[pl.ds(0, hs)], g.at[0, pl.ds(row, hs)], 4)
            y2 = rc(xt.at[pl.ds(hs, ht)], g.at[0, pl.ds(row + hs, ht)], 4)
            x1 = rc(xt.at[pl.ds(hs, ht)], g.at[2, pl.ds(row + hs, ht)], 2)
            x2 = rc(xt.at[pl.ds(0, hs)], g.at[2, pl.ds(row, hs)], 2)
            c0 = rc(xt, g.at[1, pl.ds(row, seq)], 1)
            start(y1, x1, y2, x2, c0, *lnc)
            wl = load_out(0)
            first_weights = load_first(0)
            waitl(wl)
            turn_out()
            y1.wait_recv()
            rx = rc(g.at[0, pl.ds(orow, hs)], g.at[2, pl.ds(orow, hs)], 2)
            rx.start()
            x1.wait_recv()
            ry = rc(g.at[2, pl.ds(row + hs, ht)], g.at[2, pl.ds(row + hs, ht)], 4)
            ry.start()
            y2.wait_recv()
            c1 = rc(g.at[0, pl.ds(orow, seq)], g.at[1, pl.ds(orow, seq)], 1)
            c1.start()
            sent.extend([y1, y2, x1, x2, c0, rx, ry, c1])

            def rest():
                x2.wait_recv()
                c2 = rc(g.at[2, pl.ds(row, seq)], g.at[3, pl.ds(row, seq)], 1)
                c2.start()
                recvs([rx, ry])
                c3 = rc(g.at[2, pl.ds(orow, seq)], g.at[3, pl.ds(orow, seq)], 1)
                c3.start()
                sent.extend([c2, c3])
                return [c2, c3]
            return rest, [c0, c1], first_weights

        def tile_cols(t, base=0):
            off = base + t * tile
            return pl.ds(off if isinstance(off, int) else pl.multiple_of(off, tile), tile)

        def gather1(l, finish):
            g = xg_ref.at[l]
            lo, hi = pl.ds(0, 304), pl.ds(304, two - 304)
            ys, xs, own = [], [], []

            def send(t):
                src, dc = nbuf.at[:, tile_cols(t)], tile_cols(t, ycol)
                ys.append(rc(src, g.at[0, :, dc], 4))
                xs.append(rc(src, g.at[2, :, dc], 2))
                own.append(lc(src, g.at[0, :, dc]))
                start(ys[t], xs[t], own[t])
            for t in range(out_tiles):
                finish(t)
                if t:
                    send(t - 1)
            send(out_tiles - 1)
            rx, ry = [], []
            for t in range(out_tiles):
                ys[t].wait_recv()
                oc = tile_cols(t, ocol)
                rx.append(rc(g.at[0, lo, oc], g.at[2, lo, oc], 2))
                rx[t].start()
            waitl(own)
            c1 = rc(g.at[0], g.at[1], 1)
            c1.start()
            for t in range(out_tiles):
                xs[t].wait_recv()
                yc = tile_cols(t, ycol)
                ry.append(rc(g.at[2, hi, yc], g.at[2, hi, yc], 4))
                ry[t].start()
            sent.extend(ys + xs + rx + ry + [c1])

            def rest():
                recvs(rx + ry)
                c3 = rc(g.at[2], g.at[3], 1)
                c3.start()
                sent.append(c3)
                return [c3]
            return rest, [c1]

        def send_weights(l):
            rows = pl.ds(pl.multiple_of(cc * q, 64), cc)
            out = []
            for r in (2, 3, 1):
                t = flip(me, r)
                ty = flip(t, 4)
                out.append(rc(wd_ref.at[l, :, pl.ds(pl.multiple_of(hid * t, 128), hid)], w2_ref.at[l, rows, pl.ds(0, hid)], r))
                out.append(rc(wd_ref.at[l, :, pl.ds(pl.multiple_of(hid * ty, 128), hid)], w2_ref.at[l, rows, pl.ds(hid, hid)], r))
                out.append(rc(wot.at[t % 4], w2_ref.at[l, rows, pl.ds(2 * hid, 2 * cc)], r))
            start(*out)
            sent.extend(out)
            return out

        def own_weights(l):
            rows = pl.ds(pl.multiple_of(cc * q, 64), cc)
            return start(
                lc(wd_ref.at[l, :, pl.ds(pl.multiple_of(hid * me, 128), hid)], w2v.at[rows, pl.ds(0, hid)]),
                lc(wd_ref.at[l, :, pl.ds(pl.multiple_of(hid * flip(me, 4), 128), hid)], w2v.at[rows, pl.ds(hid, hid)]))

        def other_weights(l, inbound):
            recvs(inbound)
            cs = []
            for r in (1, 2, 3):
                rows = pl.ds(pl.multiple_of(cc * flip(q, r), 64), cc)
                cs.append(lc(w2_ref.at[l, rows], w2v.at[rows]))
            return start(*cs)

        def load_x(l, r):
            if l == 0 and r == 0:
                return start(lc(x_ref, xbuf.at[pl.ds(row, seq)]), lc(xg_ref.at[0, 0, pl.ds(orow, seq)], xbuf.at[pl.ds(orow, seq)]))
            return start(lc(xg_ref.at[l, r], xbuf))

        def norm(l):
            @pl.loop(0, two // 16, unroll=4)
            def _(i):
                rs = pl.ds(pl.multiple_of(i * 16, 16), 16)
                v = xbuf[rs, :].astype(F32)
                cen = v - jnp.mean(v, axis=-1, keepdims=True)
                var = jnp.mean(cen * cen, axis=-1, keepdims=True)
                nrm = cen * lax.rsqrt(var + EPSILON)
                k = 4 * l
                abuf[rs, :] = (nrm * lnf[k:k + 1, :] + lnf[k + 1:k + 2, :]).astype(BF16)
                mbuf[rs, :] = (nrm * lnf[k + 2:k + 3, :] + lnf[k + 3:k + 4, :]).astype(BF16)

        def h_copy(l, r, t, base):
            cs = pl.ds(pl.multiple_of(t * tile, tile), tile)
            return rc(hbuf.at[r, :, cs], hrec_ref.at[l, r, :, cs], 4, base + t)

        def up(l, r, base, now):
            @pl.loop(0, hid_tiles)
            def _(t):
                cs = pl.ds(pl.multiple_of(t * tile, tile), tile)
                u = jnp.dot(mbuf[...], wu[:, cs], preferred_element_type=F32)
                hbuf[r, :, cs] = (0.5 * u * (1.0 + lax.erf(u * (0.5 ** 0.5)))).astype(BF16)

                @pl.when((t > 0) & (t <= now))
                def _():
                    h_copy(l, r, t - 1, base).start()
            if now == hid_tiles:
                h_copy(l, r, hid_tiles - 1, base).start()

        def attend(l, r):
            kidx = lax.broadcasted_iota(jnp.int32, (seq, seq), 0)
            qidx = lax.broadcasted_iota(jnp.int32, (seq, seq), 1)
            causal = kidx <= qidx
            kf = kidx.astype(F32)

            @pl.loop(0, heads)
            def _(h):
                t = lax.dot_general(wq[pl.ds(pl.multiple_of(h * slot, 16), slot), :], abuf[...], NT, preferred_element_type=F32)
                t = t.astype(BF16).astype(F32)
                cs, sn = cos_ref[...], sin_ref[...]

                def turn(v):
                    a, b = v[:half_hd], v[half_hd:]
                    return jnp.concatenate([a * cs - b * sn, b * cs + a * sn], axis=0).astype(BF16)
                qr, kr, vr = turn(t[:hd]), turn(t[hd:2 * hd]), t[2 * hd:].astype(BF16)
                hrow = pl.ds(pl.multiple_of(h * hd, 16), hd)
                kvb[r, 0, hrow, :] = kr
                kvb[r, 1, hrow, :] = vr
                crow = pl.ds(pl.multiple_of(cc * yb + h * hd, 16), hd)
                for j in range(2):
                    ps = slice(j * seq, (j + 1) * seq)
                    s = lax.dot_general(kr[:, ps], qr[:, ps], TN, preferred_element_type=F32) * hd ** -0.5
                    plen = lnrec[flip(q, r) + 4 * j, 8:9, 0:seq].astype(F32)
                    s = jnp.where(causal & (kf < plen), s, -1e30)
                    e = jnp.exp(s - jnp.max(s, axis=0, keepdims=True))
                    p = (e / jnp.sum(e, axis=0, keepdims=True)).astype(BF16)
                    cbuf[r, crow, ps] = jnp.dot(vr[:, ps], p, preferred_element_type=F32).astype(BF16)

        def first(l, r, prev, now):
            xs = load_x(l, r)
            if prev:
                waits(prev)
            waitl(xs)
            norm(l)
            base = take(hid_tiles)
            up(l, r, base, now)
            attend(l, r)
            crows = pl.ds(pl.multiple_of(cc * yb, 64), cc)
            c = rc(cbuf.at[r, crows], crec_ref.at[l, r], 4)
            hcs = [h_copy(l, r, t, base) for t in range(hid_tiles)]
            if now == hid_tiles:
                c.start()
            return hcs, c

        def kv_send(l, r, ys):
            j = yb if ys == 0 else 1 - yb
            s = 4 * ys + r
            out = []
            for i, ref in enumerate((k_ref, v_ref)):
                src = kvb.at[r, i, :, pl.ds(pl.multiple_of(seq * j, seq), seq)]
                dst = ref.at[l, pl.ds(pl.multiple_of(cc * me, 64), cc), :]
                out.append(lc(src, dst) if s == 0 else rc(src, dst, s))
            start(*out)
            return out

        def second(l, r, hcs, c, dst, send_to, wait_before):
            recvs(hcs)
            c.wait_recv()
            orows = pl.ds(pl.multiple_of(cc * (1 - yb), 64), cc)
            cs = start(lc(hrec_ref.at[l, r], hr), lc(crec_ref.at[l, r], cbuf.at[r, orows]))
            waitl(cs)
            if wait_before:
                waits(wait_before)
            base = take(out_tiles) if send_to is not None else None

            def p_copy(t):
                ts = pl.ds(pl.multiple_of(t * tile, tile), tile)
                return rc(dst.at[:, ts], send_to.at[:, ts], 1, base + t)

            @pl.loop(0, out_tiles)
            def _(t):
                ts = pl.ds(pl.multiple_of(t * tile, tile), tile)
                acc = lax.dot_general(hbuf[r], w2v[ts, 0:hid], NT, preferred_element_type=F32)
                acc = acc + lax.dot_general(hr[...], w2v[ts, hid:2 * hid], NT, preferred_element_type=F32)
                acc = acc + lax.dot_general(cbuf[r], w2v[ts, 2 * hid:], TT, preferred_element_type=F32)
                dst[:, ts] = acc
                if send_to is not None:
                    @pl.when(t > 0)
                    def _():
                        p_copy(t - 1).start()
            if send_to is None:
                return []
            p_copy(out_tiles - 1).start()
            return [p_copy(t) for t in range(out_tiles)]

        rest, near, lw = gather0()
        res0 = start(lc(x_ref.at[:, pl.ds(ycol, half_d)], nbuf.at[pl.ds(row, seq)]),
                     lc(xg_ref.at[0, 0, pl.ds(orow, seq), pl.ds(ycol, half_d)], nbuf.at[pl.ds(orow, seq)]))
        recvs(lnc)
        lnf[...] = jnp.zeros_like(lnf)
        for e in range(n):
            lo = ncols * e - 64 * (e % 2)
            lnf[:, lo:lo + win] += lnrec[e].astype(F32)
        wait_prev = {r: [] for r in range(4)}
        p_prev = {'p2': [], 'p31': []}
        for l in range(layers):
            last = l + 1 == layers
            inbound = send_weights(l)
            w_own = own_weights(l)
            w2v[pl.ds(pl.multiple_of(cc * q, 64), cc), 2 * hid:] = wot[q]
            waitl(lw)
            hc, xc = {}, {}
            hc[0], xc[0] = first(l, 0, wait_prev[0], HELD)
            far = rest()
            hc[2], xc[2] = first(l, 2, wait_prev[2], hid_tiles)
            recvs(far)
            hc[3], xc[3] = first(l, 3, wait_prev[3], hid_tiles)
            start(*hc[0][HELD:], xc[0])
            kvs = kv_send(l, 2, 0) + kv_send(l, 3, 0) + (kv_send(l, 2, 1) if last else [])
            recvs(near)
            hc[1], xc[1] = first(l, 1, wait_prev[1], hid_tiles)
            for r in range(2 if last else 4):
                kvs += kv_send(l, r, 1)
            kvs += kv_send(l, 1, 0)
            loc = kv_send(l, 0, 0)
            if not last:
                lw = load_first(l + 1)
                lwo = load_out(l + 1)
            w_in = other_weights(l, inbound)
            waitl(w_own)
            waitl(w_in)
            second(l, 2, hc[2], xc[2], p2, None, p_prev['p2'])
            c3 = second(l, 3, hc[3], xc[3], p31, pd3, p_prev['p31'])
            xcs = []
            for t in range(out_tiles):
                ts = slice(t * tile, (t + 1) * tile)
                c3[t].wait_recv()
                p2[:, ts] += pd3[:, ts]
                xcs.append(rc(p2.at[:, tile_cols(t)], px.at[:, tile_cols(t)], 2))
                if t:
                    xcs[t - 1].start()
            xcs[-1].start()
            second(l, 0, hc[0], xc[0], p0, None, [])
            c1 = second(l, 1, hc[1], xc[1], p31, pd1, c3)
            if l == 0:
                waitl(res0)
            waits(sent)
            sent.clear()
            if not last:
                waitl(lwo)
                turn_out()

            def finish(t):
                ts = slice(t * tile, (t + 1) * tile)
                c1[t].wait_recv()
                xcs[t].wait_recv()
                total = p0[:, ts] + pd1[:, ts] + px[:, ts]
                nbuf[:, ts] = (nbuf[:, ts].astype(F32) + total).astype(BF16)

            if not last:
                rest, near = gather1(l + 1, finish)
                wait_prev = {r: hc[r] + [xc[r]] for r in range(4)}
                wait_prev[0] = wait_prev[0] + kvs
                p_prev = {'p2': xcs, 'p31': c1}
                waitl(loc)
                kv_in = kvs
            else:
                fin, own = [], []

                def send(t):
                    dc = tile_cols(t, ycol)
                    fin.append(rc(nbuf.at[pl.ds(orow, seq), tile_cols(t)], y_ref.at[:, dc], 4))
                    own.append(lc(nbuf.at[pl.ds(row, seq), tile_cols(t)], y_ref.at[:, dc]))
                    start(fin[t], own[t])
                for t in range(out_tiles):
                    finish(t)
                    if t:
                        send(t - 1)
                send(out_tiles - 1)
                kvs += kv_send(l, 3, 1)
                waits(xcs + c1 + [c for r in range(4) for c in hc[r] + [xc[r]]] + kvs + fin)
                recvs(kv_in + kvs + fin)
                waitl(own + loc)
        waits(lnc)
        assert counter[0] <= cfg['n_remote'] and counter[1] <= cfg['n_local'], counter
    return kernel


def hand_over(parts):
    def kernel(*refs):
        srcs, dsts = refs[:3], refs[3:6]
        bufs, rsem, wsem = refs[6:9], refs[9], refs[10]
        pieces = []
        for a in range(3):
            rows = srcs[a].shape[0] // parts[a]
            for i in range(parts[a]):
                pieces.append((a, pl.ds(i * rows, rows)))
        reads = [pltpu.make_async_copy(srcs[a].at[rs], bufs[a].at[rs], rsem.at[i]) for i, (a, rs) in enumerate(pieces)]
        writes = [pltpu.make_async_copy(bufs[a].at[rs], dsts[a].at[rs], wsem.at[i]) for i, (a, rs) in enumerate(pieces)]
        for c in reads:
            c.start()
        for r, w in zip(reads, writes):
            r.wait()
            w.start()
        for w in writes:
            w.wait()

    def call(*arrays):
        hbm = pl.BlockSpec(memory_space=pltpu.MemorySpace.HBM)
        total = sum(parts)
        return pl.pallas_call(
            kernel,
            out_shape=[jax.ShapeDtypeStruct(a.shape, a.dtype) for a in arrays],
            in_specs=[hbm] * 3, out_specs=[hbm] * 3,
            scratch_shapes=[pltpu.VMEM(a.shape, a.dtype) for a in arrays] + [pltpu.SemaphoreType.DMA((total,)), pltpu.SemaphoreType.DMA((total,))],
        )(*arrays)
    return call


def solution(mesh):
    n = mesh.shape['wg']
    batch_spec = P(('dp', 'wg'))
    col_spec = P(None, None, 'wg')
    out_spec = P(None, None, None, 'wg')
    cache_spec = P(None, ('dp', 'wg'))

    def local_program(x, positions, prompt_len, ln_attn, ln_mlp, w_qkv, w_out, w_up, w_down):
        layers, d, _ = w_qkv.shape
        n_heads, hd = w_out.shape[1], w_out.shape[2]
        heads = n_heads // n
        seq, hid, cc = x.shape[1], w_up.shape[2], heads * hd
        two, half_d = 2 * seq, d // 2
        me = lax.axis_index('wg')
        cfg = dict(n=n, layers=layers, seq=seq, d=d, heads=heads, hd=hd, hid=hid, n_remote=192, n_local=96)
        half_hd = hd // 2
        inv_freq = (ROPE_BASE ** (-np.arange(half_hd) * 2.0 / hd)).astype(np.float32)
        freq = jnp.asarray(inv_freq[:, None])
        win = d // n + 64
        wq_t = w_qkv.transpose(0, 2, 1)
        wd_t = w_down.transpose(0, 2, 1)
        wo_n = w_out.reshape(layers, d, -1)

        hbm = pl.BlockSpec(memory_space=pltpu.MemorySpace.HBM)
        vmem = pl.BlockSpec(memory_space=pltpu.MemorySpace.VMEM)
        sds = jax.ShapeDtypeStruct
        outs = pl.pallas_call(
            make_kernel(cfg),
            out_shape=[
                sds((seq, d), BF16), sds((layers, d, seq), BF16), sds((layers, d, seq), BF16), sds((layers, 4, two, d), BF16),
                sds((layers, half_d, 2 * hid + 2 * cc), BF16), sds((layers, 4, two, hid), BF16), sds((layers, 4, cc, two), BF16)],
            in_specs=[hbm] * 5 + [vmem, vmem, pl.BlockSpec(memory_space=pltpu.MemorySpace.SMEM), vmem, vmem],
            out_specs=[hbm] * 7,
            scratch_shapes=[
                pltpu.VMEM((3 * cc, d), BF16), pltpu.VMEM((d, hid), BF16), pltpu.VMEM((half_d, 2 * hid + 2 * cc), BF16),
                pltpu.VMEM((d, d // n), BF16), pltpu.VMEM((4, cc, 2 * cc), BF16),
                pltpu.VMEM((two, d), BF16), pltpu.VMEM((two, d), BF16), pltpu.VMEM((two, d), BF16),
                pltpu.VMEM((4, two, hid), BF16), pltpu.VMEM((two, hid), BF16),
                pltpu.VMEM((4, 2, cc, two), BF16), pltpu.VMEM((4, 2 * cc, two), BF16),
                pltpu.VMEM((two, half_d), F32), pltpu.VMEM((two, half_d), F32), pltpu.VMEM((two, half_d), F32),
                pltpu.VMEM((two, half_d), F32), pltpu.VMEM((two, half_d), F32), pltpu.VMEM((two, half_d), F32),
                pltpu.VMEM((two, half_d), BF16), pltpu.VMEM((half_hd, two), F32), pltpu.VMEM((half_hd, two), F32), pltpu.VMEM((16, win), F32), pltpu.VMEM((16, win), BF16), pltpu.VMEM((n, 16, win), BF16), pltpu.VMEM((16, d), F32),
                pltpu.SemaphoreType.DMA((cfg['n_remote'],)), pltpu.SemaphoreType.DMA((cfg['n_remote'],)),
                pltpu.SemaphoreType.DMA((cfg['n_local'],))],
            compiler_params=pltpu.CompilerParams(collective_id=0, has_side_effects=True, vmem_limit_bytes=67043328),
        )(x[0], wq_t, w_up, wd_t, wo_n, ln_attn, ln_mlp, prompt_len, positions[None, :], freq)
        y, kc, vc = hand_over((2, 4, 4))(outs[0], outs[1].reshape(layers * d, seq), outs[2].reshape(layers * d, seq))
        caches = [c.reshape(layers, 1, n_heads, hd, seq).transpose(0, 1, 4, 2, 3) for c in (kc, vc)]
        return y[None], caches[0], caches[1]

    return jax.shard_map(local_program, mesh=mesh, in_specs=(batch_spec, P('dp'), batch_spec, col_spec, col_spec, col_spec, out_spec, col_spec, col_spec), out_specs=(batch_spec, cache_spec, cache_spec), check_vma=False)
```

```python
import jax
import jax.numpy as jnp
import numpy as np
from jax import lax
from jax.experimental import pallas as pl
from jax.experimental.pallas import tpu as pltpu
from jax.sharding import PartitionSpec as P

EPSILON = 1e-5
ROPE_BASE = 10000.0
F32 = jnp.float32
BF16 = jnp.bfloat16
MESH = pl.DeviceIdType.MESH
NT = (((1,), (1,)), ((), ()))
TN = (((0,), (0,)), ((), ()))
TT = (((0,), (1,)), ((), ()))
HELD = 3


def flip(v, s):
    if s & 1:
        v = v + 1 - 2 * (v % 2)
    if s & 2:
        v = v + 2 - 4 * ((v // 2) % 2)
    if s & 4:
        v = v + 4 - 8 * ((v // 4) % 2)
    return v


def make_kernel(cfg):
    n, layers, seq, d, heads, hd, hid = (cfg[k] for k in ('n', 'layers', 'seq', 'd', 'heads', 'hd', 'hid'))
    two = 2 * seq
    cc = heads * hd
    half_d = d // 2
    hs = 112
    ht = seq - hs
    slot = 3 * hd
    half_hd = hd // 2
    tile = 256
    hid_tiles, out_tiles = hid // tile, half_d // tile
    ncols = d // n
    win = ncols + 64

    def kernel(x_ref, wq_ref, wu_ref, wd_ref, wo_ref, la_ref, lm_ref, len_ref, pos_ref, freq_ref,
               y_ref, k_ref, v_ref, xg_ref, w2_ref, hrec_ref, crec_ref,
               wq, wu, w2v, wob, wot, xbuf, abuf, mbuf, hbuf, hr, kvb, cbuf, p2, p31, p0, pd3, pd1, px, nbuf, cos_ref, sin_ref, lnst, lnsend, lnrec, lnf,
               ssem, rsem, lsem):
        me = lax.axis_index('wg')
        yb = me // 4
        q = me % 4
        row = pl.multiple_of(seq * yb, seq)
        orow = pl.multiple_of(seq * (1 - yb), seq)
        ycol = pl.multiple_of(half_d * yb, half_d)
        ocol = pl.multiple_of(half_d * (1 - yb), half_d)
        counter = [0, 0]

        def take(k=1):
            counter[0] += k
            return counter[0] - k

        def rc(src, dst, s, idx=None):
            i = take() if idx is None else idx
            return pltpu.make_async_remote_copy(src_ref=src, dst_ref=dst, send_sem=ssem.at[i], recv_sem=rsem.at[i],
                                                device_id={'wg': flip(me, s)}, device_id_type=MESH)

        def lc(src, dst):
            counter[1] += 1
            return pltpu.make_async_copy(src, dst, lsem.at[counter[1] - 1])

        def start(*cs):
            for c in cs:
                c.start()
            return cs

        def waits(cs):
            for c in cs:
                c.wait_send()

        def recvs(cs):
            for c in cs:
                c.wait_recv()

        def waitl(cs):
            for c in cs:
                c.wait()

        barrier = pltpu.get_barrier_semaphore()
        for s in range(1, n):
            pl.semaphore_signal(barrier, inc=1, device_id={'wg': flip(me, s)}, device_id_type=MESH)

        angles = freq_ref[...] * pos_ref[...].astype(F32)
        for f, ref in ((jnp.cos, cos_ref), (jnp.sin, sin_ref)):
            ref[:, 0:seq] = f(angles)
            ref[:, seq:two] = ref[:, 0:seq]

        lnst[...] = jnp.zeros_like(lnst)
        for i in range(layers):
            lnst[4 * i:4 * i + 2, 0:ncols] = la_ref[i].astype(F32)
            lnst[4 * i + 2:4 * i + 4, 0:ncols] = lm_ref[i].astype(F32)
        moved = jnp.where(me % 2 == 1, pltpu.roll(lnst[...], 64, 1), lnst[...])
        is_len = lax.broadcasted_iota(jnp.int32, (16, win), 0) == 4 * layers
        lnsend[...] = jnp.where(is_len, len_ref[0].astype(F32), moved).astype(BF16)
        lnrec[me] = lnsend[...]
        pl.semaphore_wait(barrier, n - 1)

        sent = []
        lnc = [rc(lnsend, lnrec.at[me], s) for s in range(1, n)]

        def load_out(l):
            return start(lc(wo_ref.at[l], wob))

        def turn_out():
            eye = (lax.broadcasted_iota(jnp.int32, (cc, cc), 0) == lax.broadcasted_iota(jnp.int32, (cc, cc), 1)).astype(F32).astype(BF16)
            for i in range(4):
                pair = jnp.concatenate([wob[cc * i:cc * (i + 1), :], wob[cc * (i + 4):cc * (i + 5), :]], axis=0)
                wot[i] = lax.dot_general(eye, pair, NT, preferred_element_type=F32).astype(BF16)

        def load_first(l):
            return start(lc(wq_ref.at[l], wq), lc(wu_ref.at[l], wu))

        def gather0():
            xt, g = x_ref, xg_ref.at[0]
            y1 = rc(xt.at[pl.ds(0, hs)], g.at[0, pl.ds(row, hs)], 4)
            y2 = rc(xt.at[pl.ds(hs, ht)], g.at[0, pl.ds(row + hs, ht)], 4)
            x1 = rc(xt.at[pl.ds(hs, ht)], g.at[2, pl.ds(row + hs, ht)], 2)
            x2 = rc(xt.at[pl.ds(0, hs)], g.at[2, pl.ds(row, hs)], 2)
            c0 = rc(xt, g.at[1, pl.ds(row, seq)], 1)
            start(y1, x1, y2, x2, c0, *lnc)
            wl = load_out(0)
            first_weights = load_first(0)
            waitl(wl)
            turn_out()
            y1.wait_recv()
            rx = rc(g.at[0, pl.ds(orow, hs)], g.at[2, pl.ds(orow, hs)], 2)
            rx.start()
            x1.wait_recv()
            ry = rc(g.at[2, pl.ds(row + hs, ht)], g.at[2, pl.ds(row + hs, ht)], 4)
            ry.start()
            y2.wait_recv()
            c1 = rc(g.at[0, pl.ds(orow, seq)], g.at[1, pl.ds(orow, seq)], 1)
            c1.start()
            sent.extend([y1, y2, x1, x2, c0, rx, ry, c1])

            def rest():
                x2.wait_recv()
                c2 = rc(g.at[2, pl.ds(row, seq)], g.at[3, pl.ds(row, seq)], 1)
                c2.start()
                recvs([rx, ry])
                c3 = rc(g.at[2, pl.ds(orow, seq)], g.at[3, pl.ds(orow, seq)], 1)
                c3.start()
                sent.extend([c2, c3])
                return [c2, c3]
            return rest, [c0, c1], first_weights

        def tile_cols(t, base=0):
            off = base + t * tile
            return pl.ds(off if isinstance(off, int) else pl.multiple_of(off, tile), tile)

        def gather1(l, finish):
            g = xg_ref.at[l]
            lo, hi = pl.ds(0, 304), pl.ds(304, two - 304)
            ys, xs, own = [], [], []

            def send(t):
                src, dc = nbuf.at[:, tile_cols(t)], tile_cols(t, ycol)
                ys.append(rc(src, g.at[0, :, dc], 4))
                xs.append(rc(src, g.at[2, :, dc], 2))
                own.append(lc(src, g.at[0, :, dc]))
                start(ys[t], xs[t], own[t])
            for t in range(out_tiles):
                finish(t)
                if t:
                    send(t - 1)
            send(out_tiles - 1)
            rx, ry = [], []
            for t in range(out_tiles):
                ys[t].wait_recv()
                oc = tile_cols(t, ocol)
                rx.append(rc(g.at[0, lo, oc], g.at[2, lo, oc], 2))
                rx[t].start()
            waitl(own)
            c1 = rc(g.at[0], g.at[1], 1)
            c1.start()
            for t in range(out_tiles):
                xs[t].wait_recv()
                yc = tile_cols(t, ycol)
                ry.append(rc(g.at[2, hi, yc], g.at[2, hi, yc], 4))
                ry[t].start()
            sent.extend(ys + xs + rx + ry + [c1])

            def rest():
                recvs(rx + ry)
                c3 = rc(g.at[2], g.at[3], 1)
                c3.start()
                sent.append(c3)
                return [c3]
            return rest, [c1]

        def send_weights(l):
            rows = pl.ds(pl.multiple_of(cc * q, 64), cc)
            out = []
            for r in (2, 3, 1):
                t = flip(me, r)
                ty = flip(t, 4)
                out.append(rc(wd_ref.at[l, :, pl.ds(pl.multiple_of(hid * t, 128), hid)], w2_ref.at[l, rows, pl.ds(0, hid)], r))
                out.append(rc(wd_ref.at[l, :, pl.ds(pl.multiple_of(hid * ty, 128), hid)], w2_ref.at[l, rows, pl.ds(hid, hid)], r))
                out.append(rc(wot.at[t % 4], w2_ref.at[l, rows, pl.ds(2 * hid, 2 * cc)], r))
            start(*out)
            sent.extend(out)
            return out

        def own_weights(l):
            rows = pl.ds(pl.multiple_of(cc * q, 64), cc)
            return start(
                lc(wd_ref.at[l, :, pl.ds(pl.multiple_of(hid * me, 128), hid)], w2v.at[rows, pl.ds(0, hid)]),
                lc(wd_ref.at[l, :, pl.ds(pl.multiple_of(hid * flip(me, 4), 128), hid)], w2v.at[rows, pl.ds(hid, hid)]))

        def other_weights(l, inbound):
            recvs(inbound)
            cs = []
            for r in (1, 2, 3):
                rows = pl.ds(pl.multiple_of(cc * flip(q, r), 64), cc)
                cs.append(lc(w2_ref.at[l, rows], w2v.at[rows]))
            return start(*cs)

        def load_x(l, r):
            if l == 0 and r == 0:
                return start(lc(x_ref, xbuf.at[pl.ds(row, seq)]), lc(xg_ref.at[0, 0, pl.ds(orow, seq)], xbuf.at[pl.ds(orow, seq)]))
            return start(lc(xg_ref.at[l, r], xbuf))

        def norm(l):
            @pl.loop(0, two // 16, unroll=4)
            def _(i):
                rs = pl.ds(pl.multiple_of(i * 16, 16), 16)
                v = xbuf[rs, :].astype(F32)
                cen = v - jnp.mean(v, axis=-1, keepdims=True)
                var = jnp.mean(cen * cen, axis=-1, keepdims=True)
                nrm = cen * lax.rsqrt(var + EPSILON)
                k = 4 * l
                abuf[rs, :] = (nrm * lnf[k:k + 1, :] + lnf[k + 1:k + 2, :]).astype(BF16)
                mbuf[rs, :] = (nrm * lnf[k + 2:k + 3, :] + lnf[k + 3:k + 4, :]).astype(BF16)

        def h_copy(l, r, t, base):
            cs = pl.ds(pl.multiple_of(t * tile, tile), tile)
            return rc(hbuf.at[r, :, cs], hrec_ref.at[l, r, :, cs], 4, base + t)

        def up(l, r, base, now):
            @pl.loop(0, hid_tiles)
            def _(t):
                cs = pl.ds(pl.multiple_of(t * tile, tile), tile)
                u = jnp.dot(mbuf[...], wu[:, cs], preferred_element_type=F32)
                hbuf[r, :, cs] = (0.5 * u * (1.0 + lax.erf(u * (0.5 ** 0.5)))).astype(BF16)

                @pl.when((t > 0) & (t <= now))
                def _():
                    h_copy(l, r, t - 1, base).start()
            if now == hid_tiles:
                h_copy(l, r, hid_tiles - 1, base).start()

        def attend(l, r):
            kidx = lax.broadcasted_iota(jnp.int32, (seq, seq), 0)
            qidx = lax.broadcasted_iota(jnp.int32, (seq, seq), 1)
            causal = kidx <= qidx
            kf = kidx.astype(F32)

            @pl.loop(0, heads)
            def _(h):
                t = lax.dot_general(wq[pl.ds(pl.multiple_of(h * slot, 16), slot), :], abuf[...], NT, preferred_element_type=F32)
                t = t.astype(BF16).astype(F32)
                cs, sn = cos_ref[...], sin_ref[...]

                def turn(v):
                    a, b = v[:half_hd], v[half_hd:]
                    return jnp.concatenate([a * cs - b * sn, b * cs + a * sn], axis=0).astype(BF16)
                qr, kr, vr = turn(t[:hd]), turn(t[hd:2 * hd]), t[2 * hd:].astype(BF16)
                hrow = pl.ds(pl.multiple_of(h * hd, 16), hd)
                kvb[4 * l + r, 0, hrow, :] = kr
                kvb[4 * l + r, 1, hrow, :] = vr
                crow = pl.ds(pl.multiple_of(cc * yb + h * hd, 16), hd)
                for j in range(2):
                    ps = slice(j * seq, (j + 1) * seq)
                    s = lax.dot_general(kr[:, ps], qr[:, ps], TN, preferred_element_type=F32) * hd ** -0.5
                    plen = lnrec[flip(q, r) + 4 * j, 8:9, 0:seq].astype(F32)
                    s = jnp.where(causal & (kf < plen), s, -1e30)
                    e = jnp.exp(s - jnp.max(s, axis=0, keepdims=True))
                    p = (e / jnp.sum(e, axis=0, keepdims=True)).astype(BF16)
                    cbuf[r, crow, ps] = jnp.dot(vr[:, ps], p, preferred_element_type=F32).astype(BF16)

        def first(l, r, prev, now):
            xs = load_x(l, r)
            if prev:
                waits(prev)
            waitl(xs)
            norm(l)
            base = take(hid_tiles)
            up(l, r, base, now)
            attend(l, r)
            crows = pl.ds(pl.multiple_of(cc * yb, 64), cc)
            c = rc(cbuf.at[r, crows], crec_ref.at[l, r], 4)
            hcs = [h_copy(l, r, t, base) for t in range(hid_tiles)]
            if now == hid_tiles:
                c.start()
            return hcs, c

        def kv_send(l, r, ys):
            j = yb if ys == 0 else 1 - yb
            s = 4 * ys + r
            out = []
            for i, ref in enumerate((k_ref, v_ref)):
                src = kvb.at[4 * l + r, i, :, pl.ds(pl.multiple_of(seq * j, seq), seq)]
                dst = ref.at[l, pl.ds(pl.multiple_of(cc * me, 64), cc), :]
                out.append(lc(src, dst) if s == 0 else rc(src, dst, s))
            start(*out)
            return out

        def second(l, r, hcs, c, dst, send_to, wait_before):
            recvs(hcs)
            c.wait_recv()
            orows = pl.ds(pl.multiple_of(cc * (1 - yb), 64), cc)
            cs = start(lc(hrec_ref.at[l, r], hr), lc(crec_ref.at[l, r], cbuf.at[r, orows]))
            waitl(cs)
            if wait_before:
                waits(wait_before)
            base = take(out_tiles) if send_to is not None else None

            def p_copy(t):
                ts = pl.ds(pl.multiple_of(t * tile, tile), tile)
                return rc(dst.at[:, ts], send_to.at[:, ts], 1, base + t)

            @pl.loop(0, out_tiles)
            def _(t):
                ts = pl.ds(pl.multiple_of(t * tile, tile), tile)
                acc = lax.dot_general(hbuf[r], w2v[ts, 0:hid], NT, preferred_element_type=F32)
                acc = acc + lax.dot_general(hr[...], w2v[ts, hid:2 * hid], NT, preferred_element_type=F32)
                acc = acc + lax.dot_general(cbuf[r], w2v[ts, 2 * hid:], TT, preferred_element_type=F32)
                dst[:, ts] = acc
                if send_to is not None:
                    @pl.when(t > 0)
                    def _():
                        p_copy(t - 1).start()
            if send_to is None:
                return []
            p_copy(out_tiles - 1).start()
            return [p_copy(t) for t in range(out_tiles)]

        rest, near, lw = gather0()
        res0 = start(lc(x_ref.at[:, pl.ds(ycol, half_d)], nbuf.at[pl.ds(row, seq)]),
                     lc(xg_ref.at[0, 0, pl.ds(orow, seq), pl.ds(ycol, half_d)], nbuf.at[pl.ds(orow, seq)]))
        recvs(lnc)
        lnf[...] = jnp.zeros_like(lnf)
        for e in range(n):
            lo = ncols * e - 64 * (e % 2)
            lnf[:, lo:lo + win] += lnrec[e].astype(F32)
        wait_prev = {r: [] for r in range(4)}
        p_prev = {'p2': [], 'p31': []}
        for l in range(layers):
            last = l + 1 == layers
            inbound = send_weights(l)
            late = []
            if l:
                for r in (2, 3):
                    late += kv_send(l - 1, r, 1)
            w_own = own_weights(l)
            w2v[pl.ds(pl.multiple_of(cc * q, 64), cc), 2 * hid:] = wot[q]
            waitl(lw)
            hc, xc = {}, {}
            hc[0], xc[0] = first(l, 0, wait_prev[0], HELD)
            far = rest()
            hc[2], xc[2] = first(l, 2, wait_prev[2], hid_tiles)
            recvs(far)
            hc[3], xc[3] = first(l, 3, wait_prev[3], hid_tiles)
            start(*hc[0][HELD:], xc[0])
            kvs = kv_send(l, 2, 0) + kv_send(l, 3, 0) + (kv_send(l, 2, 1) if last else [])
            recvs(near)
            hc[1], xc[1] = first(l, 1, wait_prev[1], hid_tiles)
            for r in range(2):
                kvs += kv_send(l, r, 1)
            kvs += kv_send(l, 1, 0)
            loc = kv_send(l, 0, 0)
            if not last:
                lw = load_first(l + 1)
                lwo = load_out(l + 1)
            w_in = other_weights(l, inbound)
            waitl(w_own)
            waitl(w_in)
            second(l, 2, hc[2], xc[2], p2, None, p_prev['p2'])
            c3 = second(l, 3, hc[3], xc[3], p31, pd3, p_prev['p31'])
            xcs = []
            for t in range(out_tiles):
                ts = slice(t * tile, (t + 1) * tile)
                c3[t].wait_recv()
                p2[:, ts] += pd3[:, ts]
                xcs.append(rc(p2.at[:, tile_cols(t)], px.at[:, tile_cols(t)], 2))
                if t:
                    xcs[t - 1].start()
            xcs[-1].start()
            second(l, 0, hc[0], xc[0], p0, None, [])
            c1 = second(l, 1, hc[1], xc[1], p31, pd1, c3)
            if l == 0:
                waitl(res0)
            waits(sent)
            sent.clear()
            if not last:
                waitl(lwo)
                turn_out()

            def finish(t):
                ts = slice(t * tile, (t + 1) * tile)
                c1[t].wait_recv()
                xcs[t].wait_recv()
                total = p0[:, ts] + pd1[:, ts] + px[:, ts]
                nbuf[:, ts] = (nbuf[:, ts].astype(F32) + total).astype(BF16)

            if not last:
                rest, near = gather1(l + 1, finish)
                wait_prev = {r: hc[r] + [xc[r]] for r in range(4)}
                p_prev = {'p2': xcs, 'p31': c1}
                waitl(loc)
                kv_in = kvs
            else:
                fin, own = [], []

                def send(t):
                    dc = tile_cols(t, ycol)
                    fin.append(rc(nbuf.at[pl.ds(orow, seq), tile_cols(t)], y_ref.at[:, dc], 4))
                    own.append(lc(nbuf.at[pl.ds(row, seq), tile_cols(t)], y_ref.at[:, dc]))
                    start(fin[t], own[t])
                for t in range(out_tiles):
                    finish(t)
                    if t:
                        send(t - 1)
                send(out_tiles - 1)
                kvs += kv_send(l, 3, 1)
                kvs += kv_in + late
                waits(xcs + c1 + [c for r in range(4) for c in hc[r] + [xc[r]]] + kvs + fin)
                recvs(kvs + fin)
                waitl(own + loc)
        waits(lnc)
        assert counter[0] <= cfg['n_remote'] and counter[1] <= cfg['n_local'], counter
    return kernel


def hand_over(parts):
    def kernel(*refs):
        srcs, dsts = refs[:3], refs[3:6]
        bufs, rsem, wsem = refs[6:9], refs[9], refs[10]
        pieces = []
        for a in range(3):
            rows = srcs[a].shape[0] // parts[a]
            for i in range(parts[a]):
                pieces.append((a, pl.ds(i * rows, rows)))
        reads = [pltpu.make_async_copy(srcs[a].at[rs], bufs[a].at[rs], rsem.at[i]) for i, (a, rs) in enumerate(pieces)]
        writes = [pltpu.make_async_copy(bufs[a].at[rs], dsts[a].at[rs], wsem.at[i]) for i, (a, rs) in enumerate(pieces)]
        for c in reads:
            c.start()
        for r, w in zip(reads, writes):
            r.wait()
            w.start()
        for w in writes:
            w.wait()

    def call(*arrays):
        hbm = pl.BlockSpec(memory_space=pltpu.MemorySpace.HBM)
        total = sum(parts)
        return pl.pallas_call(
            kernel,
            out_shape=[jax.ShapeDtypeStruct(a.shape, a.dtype) for a in arrays],
            in_specs=[hbm] * 3, out_specs=[hbm] * 3,
            scratch_shapes=[pltpu.VMEM(a.shape, a.dtype) for a in arrays] + [pltpu.SemaphoreType.DMA((total,)), pltpu.SemaphoreType.DMA((total,))],
        )(*arrays)
    return call


def solution(mesh):
    n = mesh.shape['wg']
    batch_spec = P(('dp', 'wg'))
    col_spec = P(None, None, 'wg')
    out_spec = P(None, None, None, 'wg')
    cache_spec = P(None, ('dp', 'wg'))

    def local_program(x, positions, prompt_len, ln_attn, ln_mlp, w_qkv, w_out, w_up, w_down):
        layers, d, _ = w_qkv.shape
        n_heads, hd = w_out.shape[1], w_out.shape[2]
        heads = n_heads // n
        seq, hid, cc = x.shape[1], w_up.shape[2], heads * hd
        two, half_d = 2 * seq, d // 2
        me = lax.axis_index('wg')
        cfg = dict(n=n, layers=layers, seq=seq, d=d, heads=heads, hd=hd, hid=hid, n_remote=192, n_local=96)
        half_hd = hd // 2
        inv_freq = (ROPE_BASE ** (-np.arange(half_hd) * 2.0 / hd)).astype(np.float32)
        freq = jnp.asarray(inv_freq[:, None])
        win = d // n + 64
        wq_t = w_qkv.transpose(0, 2, 1)
        wd_t = w_down.transpose(0, 2, 1)
        wo_n = w_out.reshape(layers, d, -1)

        hbm = pl.BlockSpec(memory_space=pltpu.MemorySpace.HBM)
        vmem = pl.BlockSpec(memory_space=pltpu.MemorySpace.VMEM)
        sds = jax.ShapeDtypeStruct
        outs = pl.pallas_call(
            make_kernel(cfg),
            out_shape=[
                sds((seq, d), BF16), sds((layers, d, seq), BF16), sds((layers, d, seq), BF16), sds((layers, 4, two, d), BF16),
                sds((layers, half_d, 2 * hid + 2 * cc), BF16), sds((layers, 4, two, hid), BF16), sds((layers, 4, cc, two), BF16)],
            in_specs=[hbm] * 5 + [vmem, vmem, pl.BlockSpec(memory_space=pltpu.MemorySpace.SMEM), vmem, vmem],
            out_specs=[hbm] * 7,
            scratch_shapes=[
                pltpu.VMEM((3 * cc, d), BF16), pltpu.VMEM((d, hid), BF16), pltpu.VMEM((half_d, 2 * hid + 2 * cc), BF16),
                pltpu.VMEM((d, d // n), BF16), pltpu.VMEM((4, cc, 2 * cc), BF16),
                pltpu.VMEM((two, d), BF16), pltpu.VMEM((two, d), BF16), pltpu.VMEM((two, d), BF16),
                pltpu.VMEM((4, two, hid), BF16), pltpu.VMEM((two, hid), BF16),
                pltpu.VMEM((4 * layers, 2, cc, two), BF16), pltpu.VMEM((4, 2 * cc, two), BF16),
                pltpu.VMEM((two, half_d), F32), pltpu.VMEM((two, half_d), F32), pltpu.VMEM((two, half_d), F32),
                pltpu.VMEM((two, half_d), F32), pltpu.VMEM((two, half_d), F32), pltpu.VMEM((two, half_d), F32),
                pltpu.VMEM((two, half_d), BF16), pltpu.VMEM((half_hd, two), F32), pltpu.VMEM((half_hd, two), F32), pltpu.VMEM((16, win), F32), pltpu.VMEM((16, win), BF16), pltpu.VMEM((n, 16, win), BF16), pltpu.VMEM((16, d), F32),
                pltpu.SemaphoreType.DMA((cfg['n_remote'],)), pltpu.SemaphoreType.DMA((cfg['n_remote'],)),
                pltpu.SemaphoreType.DMA((cfg['n_local'],))],
            compiler_params=pltpu.CompilerParams(collective_id=0, has_side_effects=True, vmem_limit_bytes=67043328),
        )(x[0], wq_t, w_up, wd_t, wo_n, ln_attn, ln_mlp, prompt_len, positions[None, :], freq)
        y, kc, vc = hand_over((2, 4, 4))(outs[0], outs[1].reshape(layers * d, seq), outs[2].reshape(layers * d, seq))
        caches = [c.reshape(layers, 1, n_heads, hd, seq).transpose(0, 1, 4, 2, 3) for c in (kc, vc)]
        return y[None], caches[0], caches[1]

    return jax.shard_map(local_program, mesh=mesh, in_specs=(batch_spec, P('dp'), batch_spec, col_spec, col_spec, col_spec, out_spec, col_spec, col_spec), out_specs=(batch_spec, cache_spec, cache_spec), check_vma=False)
```
